32 devices in a mesh: col: 16 (over z, y, x), row: 2 (over core).
Axes of the slice: x: 2, y: 2, z: 4, core: 2. Of those that a mesh axis runs over, the one named last changes fastest.
Arguments:
- gradient: bfloat16 [4096, 16384], P('row', 'col'), may hold values from -120 to 120
- momentum: float32 [4096, 16384], P('row', 'col'), may hold values from -6 to 6
- right_factor: float32 [16384, 256], P(('col', 'row')), may hold values from -0.046875 to 0.046875
Outputs:
- momentum_next: float32 [4096, 16384], P('row', 'col')
- right_next: float32 [16384, 256], P(('col', 'row'))
- update: bfloat16 [4096, 16384], P('row', 'col')
The draws below stay inside these ranges and needn't reach their ends.
All inputs are finite; a program needn't handle non-finite values.
Results may differ from the reference program's by a relative error of at most 0.0012.
Values sent between devices are 32-bit elements; how exact they have to be, the bound alone decides.
No kernel may reach another device: no remote copies, remote signals or barrier semaphores. Data moves between devices by JAX's collectives and lax.ppermute only.
A program may use at most 64 MiB of HBM per device.

```python
import math
import jax
import jax.numpy as jnp
from jax import lax

M = 4096
N = 16384
RANK = 256


def draw_gradient(key, part):
    keys = jax.random.split(jax.random.fold_in(key, 17), 3)
    rows = jnp.arange(M, dtype=jnp.float32) / M
    cols = jnp.arange(N, dtype=jnp.float32) / N
    row_scale = 3.0 ** (rows - 0.5) * jnp.exp(jax.random.uniform(keys[0], (M,), jnp.float32, -0.7, 0.7))
    col_scale = 3.0 ** (cols - 0.5) * jnp.exp(jax.random.uniform(keys[1], (N,), jnp.float32, -1.15, 1.15))
    base = jax.random.normal(keys[2], (M, N), jnp.float32)
    base = jnp.clip(base, -6.0, 6.0)
    return (base * row_scale[:, None] * col_scale[None, :]).astype(jnp.bfloat16)


def block_levels(key, dims, pieces, low, largest):
    loudness = 1.0
    for dim, parts in pieces:
        heights = jax.random.uniform(jax.random.fold_in(jax.random.fold_in(key, 6), dim), (parts,), jnp.float32, low / len(pieces), largest / len(pieces))
        loudness = loudness * jnp.repeat(jnp.exp(heights), dims[dim] // parts).reshape((-1,) + (1,) * (len(dims) - 1 - dim))
    return loudness


def gaussian(stream_key, extent, scale, limit, cuts=(), kind=jnp.bfloat16):
    drawn = scale * jax.random.normal(stream_key, extent, jnp.float32)
    if cuts:
        drawn = drawn * block_levels(stream_key, extent, cuts, -0.22, 0.18)
    return jnp.clip(drawn, -limit, limit).astype(kind)


def setup_inputs(seed: int = 0) -> dict:
    splits = jax.random.split(jax.random.key(seed), 4)
    gradient = draw_gradient(jax.random.fold_in(splits[3], 71), 0)
    momentum = gaussian(splits[1], (M, N), 1.0, 6.0, ((0, 2), (1, 16)), jnp.float32)
    right_factor = gaussian(splits[2], (N, RANK), N ** -0.5, 0.046875, ((0, 32),), jnp.float32)
    return dict(gradient=gradient, momentum=momentum, right_factor=right_factor)


EPS = 1e-06
FEEDBACK = 0.05

def reference(gradient, momentum, right_factor):
    highest = lax.Precision.HIGHEST
    blend = momentum + gradient.astype(jnp.float32)
    left = jnp.dot(blend.astype(jnp.float32), right_factor.astype(jnp.float32), precision=highest, preferred_element_type=jnp.float32)
    gram = jnp.dot(left.T.astype(jnp.float32), left.astype(jnp.float32), precision=highest, preferred_element_type=jnp.float32)
    lower = jnp.linalg.cholesky(gram)
    left_orth = jax.scipy.linalg.solve_triangular(lower, left.T, lower=True).T
    right = jnp.dot(blend.T.astype(jnp.float32), left_orth.astype(jnp.float32), precision=highest, preferred_element_type=jnp.float32)
    right_norm = jnp.sqrt(lax.optimization_barrier(jnp.sum(right * right, axis=0)) + EPS)
    right_next = right / right_norm[None, :]
    momentum_next = blend - FEEDBACK * jnp.dot(left_orth.astype(jnp.float32), right.T.astype(jnp.float32), precision=highest, preferred_element_type=jnp.float32)
    factor = math.sqrt(M * N / RANK)
    update = (factor * jnp.dot(left_orth.astype(jnp.float32), right_next.T.astype(jnp.float32), precision=highest, preferred_element_type=jnp.float32)).astype(jnp.bfloat16)
    return (momentum_next, right_next, update)
```

```python
import functools
import math

import jax
import jax.numpy as jnp
from jax import lax
from jax.experimental import pallas as pl
from jax.experimental.pallas import tpu as pltpu
from jax.sharding import PartitionSpec as P

EPS = 1e-06
FEEDBACK = 0.05
F32 = jnp.float32
BF16 = jnp.bfloat16


MM = (((1,), (0,)), ((), ()))
TN = (((0,), (0,)), ((), ()))
NT = (((1,), (1,)), ((), ()))


def split(x):
    high = x.astype(BF16)
    return high, (x - high.astype(F32)).astype(BF16)


def dot3(a, b, dims):
    out = lax.dot_general(a[0], b[1], dims, preferred_element_type=F32)
    out += lax.dot_general(a[1], b[0], dims, preferred_element_type=F32)
    return out + lax.dot_general(a[0], b[0], dims, preferred_element_type=F32)


def cost(us):
    return pl.CostEstimate(flops=int(us * 1e9), bytes_accessed=1 << 20, transcendentals=0)


def left_kernel(start_ref, m_ref, g_ref, r_ref, out_ref, high_ref, low_ref):
    @pl.when(pl.program_id(0) == 0)
    def _():
        high_ref[...], low_ref[...] = split(r_ref[...])

    blend = split(m_ref[...] + g_ref[...].astype(F32))
    out_ref[...] = dot3(blend, (high_ref[...], low_ref[...]), MM)


def left_rows(momentum, gradient, right_block, start, rows, block):
    cols, rank = right_block.shape
    at = lambda i, s: (s[0] + i, 0)
    return pl.pallas_call(
        left_kernel,
        grid_spec=pltpu.PrefetchScalarGridSpec(
            num_scalar_prefetch=1,
            grid=(rows // block,),
            in_specs=[
                pl.BlockSpec((block, cols), at),
                pl.BlockSpec((block, cols), at),
                pl.BlockSpec((cols, rank), lambda i, s: (0, 0)),
            ],
            out_specs=pl.BlockSpec((block, rank), lambda i, s: (i, 0)),
            scratch_shapes=[pltpu.VMEM((cols, rank), BF16), pltpu.VMEM((cols, rank), BF16)],
        ),
        out_shape=jax.ShapeDtypeStruct((rows, rank), F32),
        cost_estimate=cost(2),
        name="left_rows",
    )((start // block).reshape(1).astype(jnp.int32), momentum, gradient, right_block)


def weight_kernel(at_ref, m_ref, g_ref, a_ref, b_ref, *rest, block, half, first):
    if first:
        w_ref, gram_ref, left_ref = rest
    else:
        w_in, gram_in, _, w_ref, gram_ref, left_ref = rest
    i = pl.program_id(0)

    @pl.when(i == 0)
    def _():
        if first:
            w_ref[...] = jnp.zeros_like(w_ref)
            gram_ref[...] = jnp.zeros_like(gram_ref)
        else:
            w_ref[...] = w_in[...]
            gram_ref[...] = gram_in[...]

    @pl.when(i < half)
    def _():
        left_ref[...] = a_ref[pl.ds(pl.multiple_of(i * block, block), block), :]

    @pl.when(i >= half)
    def _():
        left_ref[...] = b_ref[pl.ds(pl.multiple_of((i - half) * block, block), block), :]

    left = split(left_ref[...])
    blend = split(m_ref[...] + g_ref[...].astype(F32))
    w_ref[...] += dot3(left, blend, TN)
    gram_ref[...] += dot3(left, left, TN)


def weight_rows(momentum, gradient, piece_a, piece_b, starts, block, carry=None):
    all_rows, cols = momentum.shape
    rows, rank = piece_a.shape
    half = rows // block
    blocks = 2 * half
    index = jnp.concatenate([starts[0] // block + jnp.arange(half), starts[1] // block + jnp.arange(half)])
    at = lambda i, s: (s[i], 0)
    whole = lambda i, s: (0, 0)
    in_specs = [
        pl.BlockSpec((block, cols), at),
        pl.BlockSpec((block, cols), at),
        pl.BlockSpec((rows, rank), whole),
        pl.BlockSpec((rows, rank), whole),
    ]
    args = [momentum, gradient, piece_a, piece_b]
    aliases = {}
    if carry is not None:
        in_specs += [
            pl.BlockSpec((rank, cols), whole),
            pl.BlockSpec((rank, rank), whole),
            pl.BlockSpec(memory_space=pl.ANY),
        ]
        args += list(carry)
        aliases = {7: 2}
    return pl.pallas_call(
        functools.partial(weight_kernel, block=block, half=half, first=carry is None),
        grid_spec=pltpu.PrefetchScalarGridSpec(
            num_scalar_prefetch=1,
            grid=(blocks,),
            in_specs=in_specs,
            out_specs=[
                pl.BlockSpec((rank, cols), whole),
                pl.BlockSpec((rank, rank), whole),
                pl.BlockSpec((block, rank), at),
            ],
        ),
        out_shape=[
            jax.ShapeDtypeStruct((rank, cols), F32),
            jax.ShapeDtypeStruct((rank, rank), F32),
            jax.ShapeDtypeStruct((all_rows, rank), F32),
        ],
        input_output_aliases=aliases,
        cost_estimate=cost(2),
        name="weight_rows",
    )(index.astype(jnp.int32), *args)


def factor_kernel(gram_ref, other_ref, out_ref, m_ref, *, n, outer):
    lanes = 128
    chunks = n // lanes
    m_ref[:, :n] = gram_ref[...] + other_ref[...]
    ri = lax.broadcasted_iota(jnp.int32, (n, n), 0)
    ci = lax.broadcasted_iota(jnp.int32, (n, n), 1)
    m_ref[:, n:] = jnp.where(ri == ci, 1.0, 0.0).astype(F32)
    sub = lax.broadcasted_iota(jnp.int32, (8, lanes), 0)
    for o in range(0, n, outer):
        end = o + outer
        live = [k for k in range(chunks) if (k + 1) * lanes > o]
        live += [k + chunks for k in range(chunks) if k * lanes < end]
        for j in range(o, end, 8):
            rest = end - j - 8
            tops = {k: m_ref[j : j + 8, k * lanes : (k + 1) * lanes] for k in live}
            tails = {k: m_ref[j + 8 : end, k * lanes : (k + 1) * lanes] for k in live} if rest else {}
            kd, off = j // lanes, j % lanes
            cols = []
            for c in range(8):
                top = jnp.broadcast_to(tops[kd][:, off + c : off + c + 1], (8, lanes))
                tail = jnp.broadcast_to(tails[kd][:, off + c : off + c + 1], (rest, lanes)) if rest else None
                cols.append((top, tail))
            for c in range(8):
                top, tail = cols[c]
                inv = lax.rsqrt(top[c : c + 1, :])
                top = top * inv
                if rest:
                    tail = tail * inv
                for k in range(c + 1, 8):
                    scale = top[k : k + 1, :]
                    tk, lk = cols[k]
                    cols[k] = (tk - top * scale, lk - tail * scale if rest else None)
                for k in live:
                    row = tops[k][c : c + 1, :] * inv
                    tops[k] = jnp.where(sub == c, row, jnp.where(sub > c, tops[k] - top * row, tops[k]))
                    if rest:
                        tails[k] = tails[k] - tail * row
            for k in live:
                m_ref[j : j + 8, k * lanes : (k + 1) * lanes] = tops[k]
                if rest:
                    m_ref[j + 8 : end, k * lanes : (k + 1) * lanes] = tails[k]
        if end < n:
            first, last = live[0] * lanes, (live[-1] + 1) * lanes
            base = (end // lanes) * lanes
            update = lax.dot_general(
                m_ref[o:end, base:n], m_ref[o:end, first:last], TN,
                precision=lax.Precision.HIGHEST, preferred_element_type=F32,
            )
            m_ref[end:n, first:last] = m_ref[end:n, first:last] - update[end - base :, :]
    out_ref[...] = jnp.where(ri >= ci, m_ref[:, n:], 0.0)


def factor_inverse(gram, other):
    n = gram.shape[0]
    return pl.pallas_call(
        functools.partial(factor_kernel, n=n, outer=64),
        out_shape=jax.ShapeDtypeStruct((n, n), F32),
        scratch_shapes=[pltpu.VMEM((n, 2 * n), F32)],
        cost_estimate=cost(9),
        name="factor_inverse",
    )(gram, other)


def right_kernel(inv_ref, w_ref, other_ref, right_ref, square_ref):
    right = dot3(split(inv_ref[...]), split(w_ref[...] + other_ref[...]), MM)
    right_ref[...] = right
    ones = jnp.ones((8, right.shape[1]), F32)
    square_ref[...] = lax.dot_general(
        ones, right * right, NT, precision=lax.Precision.HIGHEST, preferred_element_type=F32
    )


def right_part(inverse, weight, other):
    rank, cols = weight.shape
    return pl.pallas_call(
        right_kernel,
        out_shape=[jax.ShapeDtypeStruct((rank, cols), F32), jax.ShapeDtypeStruct((8, rank), F32)],
        cost_estimate=cost(2),
        name="right_part",
    )(inverse, weight, other)


def momentum_kernel(m_ref, g_ref, left_ref, inv_ref, right_ref, out_ref, orth_ref, inv_high, inv_low, right_high):
    @pl.when(pl.program_id(0) == 0)
    def _():
        inv_high[...], inv_low[...] = split(inv_ref[...])
        right_high[...] = right_ref[...].astype(BF16)

    orth = dot3(split(left_ref[...]), (inv_high[...], inv_low[...]), NT)
    orth_ref[...] = orth
    feedback = lax.dot_general(orth.astype(BF16), right_high[...], MM, preferred_element_type=F32)
    out_ref[...] = m_ref[...] + g_ref[...].astype(F32) - FEEDBACK * feedback


def momentum_rows(momentum, gradient, left, inverse, right, block):
    rows, cols = momentum.shape
    rank = left.shape[1]
    row = lambda i: (i, 0)
    whole = lambda i: (0, 0)
    return pl.pallas_call(
        momentum_kernel,
        grid=(rows // block,),
        in_specs=[
            pl.BlockSpec((block, cols), row),
            pl.BlockSpec((block, cols), row),
            pl.BlockSpec((block, rank), row),
            pl.BlockSpec((rank, rank), whole),
            pl.BlockSpec((rank, cols), whole),
        ],
        out_specs=[pl.BlockSpec((block, cols), row), pl.BlockSpec((block, rank), row)],
        out_shape=[jax.ShapeDtypeStruct((rows, cols), F32), jax.ShapeDtypeStruct((rows, rank), F32)],
        scratch_shapes=[pltpu.VMEM((rank, rank), BF16), pltpu.VMEM((rank, rank), BF16), pltpu.VMEM((rank, cols), BF16)],
        cost_estimate=cost(8),
        name="momentum_rows",
    )(momentum, gradient, left, inverse, right)


def update_kernel(orth_ref, right_ref, square_ref, out_ref, high_ref, low_ref, *, factor):
    @pl.when(pl.program_id(0) == 0)
    def _():
        high_ref[...], low_ref[...] = split(right_ref[...])

    scale = factor / jnp.sqrt(square_ref[...] + EPS)
    orth = orth_ref[...] * scale[:1, :]
    out_ref[...] = dot3(split(orth), (high_ref[...], low_ref[...]), MM).astype(BF16)


def update_rows(orth, right, squares, factor, block):
    rows, rank = orth.shape
    cols = right.shape[1]
    return pl.pallas_call(
        functools.partial(update_kernel, factor=factor),
        grid=(rows // block,),
        in_specs=[
            pl.BlockSpec((block, rank), lambda i: (i, 0)),
            pl.BlockSpec((rank, cols), lambda i: (0, 0)),
            pl.BlockSpec(squares.shape, lambda i: (0, 0)),
        ],
        out_specs=pl.BlockSpec((block, cols), lambda i: (i, 0)),
        out_shape=jax.ShapeDtypeStruct((rows, cols), BF16),
        scratch_shapes=[pltpu.VMEM((rank, cols), BF16), pltpu.VMEM((rank, cols), BF16)],
        cost_estimate=cost(5),
        name="update_rows",
    )(orth, right, squares)


def swap(x, axis, size, step):
    return lax.ppermute(x, axis, [(i, i ^ step) for i in range(size)])


def row_rest(x, size):
    if size == 1:
        return jnp.zeros_like(x)
    total, step = swap(x, "row", size, 1), 2
    while step < size:
        whole = x + total
        total = total + swap(whole, "row", size, step)
        step *= 2
    return total


def groups_of(size):
    bits = size.bit_length() - 1
    groups, low = [], 2
    while low < bits:
        width = min(2, bits - low)
        groups.append((1 << low, 1 << width))
        low += width
    return groups


def scatter_sum(x, position, size):
    for step, members in groups_of(size):
        mine = (position // step) % members
        rows = x.shape[0] // members
        part = lambda k: lax.dynamic_slice_in_dim(x, k * rows, rows)
        got = [swap(part(mine ^ d), "col", size, d * step) for d in range(1, members)]
        x = part(mine)
        for piece in got:
            x = x + piece
    return x


def gather_rows(x, position, size):
    for step, members in reversed(groups_of(size)):
        mine = (position // step) % members
        pieces = [x] + [swap(x, "col", size, d * step) for d in range(1, members)]
        width = 1
        while width < members:
            odd = (mine // width) % 2 == 1
            pieces = [
                jnp.where(odd, jnp.concatenate([b, a]), jnp.concatenate([a, b]))
                for a, b in zip(pieces[0::2], pieces[1::2])
            ]
            width *= 2
        x = pieces[0]
    return x


def body(gradient, momentum, right_factor, *, cols_size, rows_size, factor):
    rows, cols = momentum.shape
    block = rows // 8
    half, quarter = rows // 2, rows // 4
    position = lax.axis_index("col")
    x, y = position % 2, (position // 2) % 2
    if rows_size == 2:
        other = swap(right_factor, "row", 2, 1)
        first = lax.axis_index("row") == 0
        right_block = jnp.where(first, jnp.concatenate([right_factor, other]), jnp.concatenate([other, right_factor]))
    else:
        right_block = lax.all_gather(right_factor, "row", axis=0, tiled=True)

    piece = lambda start: left_rows(momentum, gradient, right_block, start, quarter, block)
    send_a = piece((1 - x) * quarter)
    got_a = swap(send_a, "col", cols_size, 1)
    send_b = piece(half + (1 - y) * quarter)
    got_b = swap(send_b, "col", cols_size, 2)
    keep_a = piece(x * quarter)
    keep_b = piece(half + y * quarter)

    def part(a, b, k):
        return lax.dynamic_slice_in_dim(a, k * block, block) + lax.dynamic_slice_in_dim(b, k * block, block)

    next_a = swap(part(keep_a, got_a, 1 - y), "col", cols_size, 2)
    next_b = swap(part(keep_b, got_b, 1 - x), "col", cols_size, 1)
    own_a = part(keep_a, got_a, y) + next_a
    own_b = part(keep_b, got_b, x) + next_b
    own = jnp.concatenate([own_a.reshape(-1, block // (cols_size // 4), own_a.shape[1]),
                           own_b.reshape(-1, block // (cols_size // 4), own_b.shape[1])], axis=1)
    own = scatter_sum(own, position, cols_size)

    near = gather_rows(own, position, cols_size)
    cut = block // (cols_size // 4)
    near_a = near[:, :cut].reshape(block, -1)
    near_b = near[:, cut:].reshape(block, -1)
    side_a = swap(near_a, "col", cols_size, 2)
    side_b = swap(near_b, "col", cols_size, 1)
    pair_a = jnp.where(y == 1, jnp.concatenate([side_a, near_a]), jnp.concatenate([near_a, side_a]))
    pair_b = jnp.where(x == 1, jnp.concatenate([side_b, near_b]), jnp.concatenate([near_b, side_b]))
    far_a = swap(pair_a, "col", cols_size, 1)
    far_b = swap(pair_b, "col", cols_size, 2)
    carry = weight_rows(momentum, gradient, near_a, near_b,
                        (x * quarter + y * block, half + y * quarter + x * block), block)
    carry = weight_rows(momentum, gradient, side_a, side_b,
                        (x * quarter + (1 - y) * block, half + y * quarter + (1 - x) * block), block, carry)
    weight, gram, left = weight_rows(momentum, gradient, far_a, far_b,
                                     ((1 - x) * quarter, half + (1 - y) * quarter), block, carry)

    gram_rest = row_rest(gram, rows_size)
    weight_rest = row_rest(weight, rows_size)
    inverse = factor_inverse(gram, gram_rest)
    right, squares = right_part(inverse, weight, weight_rest)
    squares = squares[:1]
    step = 1
    while step < cols_size:
        squares = squares + swap(squares, "col", cols_size, step)
        step *= 2
    momentum_next, orth = momentum_rows(momentum, gradient, left, inverse, right, block)
    update = update_rows(orth, right, squares, factor, block)
    share = cols // rows_size
    mine = lax.dynamic_slice_in_dim(right, lax.axis_index("row") * share, share, axis=1)
    right_next = mine.T / jnp.sqrt(squares + EPS)
    return (momentum_next, right_next, update)


def solution(mesh):
    cols_size, rows_size = mesh.shape["col"], mesh.shape["row"]

    def step(gradient, momentum, right_factor):
        rows, cols = momentum.shape
        factor = math.sqrt(rows * cols / right_factor.shape[1])
        placed = (P("row", "col"), P("row", "col"), P(("col", "row"), None))
        return jax.shard_map(
            functools.partial(body, cols_size=cols_size, rows_size=rows_size, factor=factor),
            mesh=mesh,
            in_specs=placed,
            out_specs=(P("row", "col"), P(("col", "row"), None), P("row", "col")),
            check_vma=False,
        )(gradient, momentum, right_factor)

    return step
```

```python
import functools
import math

import jax
import jax.numpy as jnp
from jax import lax
from jax.experimental import pallas as pl
from jax.experimental.pallas import tpu as pltpu
from jax.sharding import PartitionSpec as P

EPS = 1e-06
FEEDBACK = 0.05
F32 = jnp.float32
BF16 = jnp.bfloat16


MM = (((1,), (0,)), ((), ()))
TN = (((0,), (0,)), ((), ()))
NT = (((1,), (1,)), ((), ()))


def split(x):
    high = x.astype(BF16)
    return high, (x - high.astype(F32)).astype(BF16)


def dot3(a, b, dims):
    (da,), (db,) = dims[0]
    left = jnp.concatenate([a[0], a[1], a[0]], axis=da)
    right = jnp.concatenate([b[0], b[0], b[1]], axis=db)
    return lax.dot_general(left, right, dims, preferred_element_type=F32)


def cost(us):
    return pl.CostEstimate(flops=int(us * 1e9), bytes_accessed=1 << 20, transcendentals=0)


def left_kernel(at_ref, m_ref, g_ref, own_ref, rest_ref, a_ref, b_ref, high_ref, low_ref, *, block, half, count):
    i = pl.program_id(0)

    @pl.when(i == 0)
    def _():
        own, share = at_ref[count], own_ref.shape[0]
        for k in range(high_ref.shape[0] // share):
            rows = pl.ds(k * share, share)

            @pl.when(own == k)
            def _():
                high_ref[rows, :], low_ref[rows, :] = split(own_ref[...])

            @pl.when(own != k)
            def _():
                high_ref[rows, :], low_ref[rows, :] = split(rest_ref[rest_rows(rest_ref, share, k), :])

    blend = split(m_ref[...] + g_ref[...].astype(F32))
    out = dot3(blend, (high_ref[...], low_ref[...]), MM)

    @pl.when(i < half)
    def _():
        a_ref[pl.ds(pl.multiple_of(i * block, block), block), :] = out

    @pl.when(i >= half)
    def _():
        b_ref[pl.ds(pl.multiple_of((i - half) * block, block), block), :] = out


def rest_rows(rest_ref, share, k):
    return pl.ds(0 if rest_ref.shape[0] == share else k * share, share)


def block_index(starts, half, block):
    steps = jnp.arange(half)
    return jnp.concatenate([starts[0] // block + steps, starts[1] // block + steps])


def left_rows(momentum, gradient, own, rest, core, cols, starts, rows, block):
    rank = own.shape[1]
    half = rows // block
    index = jnp.concatenate([block_index(starts, half, block), core.reshape(1)])
    at = lambda i, s: (s[i], 0)
    whole = lambda i, s: (0, 0)
    return pl.pallas_call(
        functools.partial(left_kernel, block=block, half=half, count=2 * half),
        grid_spec=pltpu.PrefetchScalarGridSpec(
            num_scalar_prefetch=1,
            grid=(2 * half,),
            in_specs=[
                pl.BlockSpec((block, cols), at),
                pl.BlockSpec((block, cols), at),
                pl.BlockSpec(own.shape, whole),
                pl.BlockSpec(rest.shape, whole),
            ],
            out_specs=[pl.BlockSpec((rows, rank), whole), pl.BlockSpec((rows, rank), whole)],
            scratch_shapes=[pltpu.VMEM((cols, rank), BF16), pltpu.VMEM((cols, rank), BF16)],
        ),
        out_shape=[jax.ShapeDtypeStruct((rows, rank), F32), jax.ShapeDtypeStruct((rows, rank), F32)],
        cost_estimate=cost(5),
        name="left_rows",
    )(index.astype(jnp.int32), momentum, gradient, own, rest)


def weight_kernel(at_ref, m_ref, g_ref, a_ref, b_ref, *rest, block, half, first):
    if first:
        w_ref, gram_ref, left_ref = rest
    else:
        w_in, gram_in, _, w_ref, gram_ref, left_ref = rest
    i = pl.program_id(0)

    @pl.when(i == 0)
    def _():
        if first:
            w_ref[...] = jnp.zeros_like(w_ref)
            gram_ref[...] = jnp.zeros_like(gram_ref)
        else:
            w_ref[...] = w_in[...]
            gram_ref[...] = gram_in[...]

    @pl.when(i < half)
    def _():
        left_ref[...] = a_ref[pl.ds(pl.multiple_of(i * block, block), block), :]

    @pl.when(i >= half)
    def _():
        left_ref[...] = b_ref[pl.ds(pl.multiple_of((i - half) * block, block), block), :]

    left = split(left_ref[...])
    blend = split(m_ref[...] + g_ref[...].astype(F32))
    w_ref[...] += dot3(left, blend, TN)
    gram_ref[...] += dot3(left, left, TN)


def weight_rows(momentum, gradient, piece_a, piece_b, starts, block, carry=None):
    all_rows, cols = momentum.shape
    rows, rank = piece_a.shape
    half = rows // block
    blocks = 2 * half
    index = block_index(starts, half, block)
    at = lambda i, s: (s[i], 0)
    whole = lambda i, s: (0, 0)
    in_specs = [
        pl.BlockSpec((block, cols), at),
        pl.BlockSpec((block, cols), at),
        pl.BlockSpec((rows, rank), whole),
        pl.BlockSpec((rows, rank), whole),
    ]
    args = [momentum, gradient, piece_a, piece_b]
    aliases = {}
    if carry is not None:
        in_specs += [
            pl.BlockSpec((rank, cols), whole),
            pl.BlockSpec((rank, rank), whole),
            pl.BlockSpec(memory_space=pl.ANY),
        ]
        args += list(carry)
        aliases = {7: 2}
    return pl.pallas_call(
        functools.partial(weight_kernel, block=block, half=half, first=carry is None),
        grid_spec=pltpu.PrefetchScalarGridSpec(
            num_scalar_prefetch=1,
            grid=(blocks,),
            in_specs=in_specs,
            out_specs=[
                pl.BlockSpec((rank, cols), whole),
                pl.BlockSpec((rank, rank), whole),
                pl.BlockSpec((block, rank), at),
            ],
        ),
        out_shape=[
            jax.ShapeDtypeStruct((rank, cols), F32),
            jax.ShapeDtypeStruct((rank, rank), F32),
            jax.ShapeDtypeStruct((all_rows, rank), F32),
        ],
        input_output_aliases=aliases,
        cost_estimate=cost(2),
        name="weight_rows",
    )(index.astype(jnp.int32), *args)


def factor_kernel(gram_ref, other_ref, out_ref, m_ref, *, n, outer):
    lanes = 128
    chunks = n // lanes
    m_ref[:, :n] = gram_ref[...] + other_ref[...]
    ri = lax.broadcasted_iota(jnp.int32, (n, n), 0)
    ci = lax.broadcasted_iota(jnp.int32, (n, n), 1)
    m_ref[:, n:] = jnp.where(ri == ci, 1.0, 0.0).astype(F32)
    sub = lax.broadcasted_iota(jnp.int32, (8, lanes), 0)
    for o in range(0, n, outer):
        end = o + outer
        live = [k for k in range(chunks) if (k + 1) * lanes > o]
        live += [k + chunks for k in range(chunks) if k * lanes < end]
        for j in range(o, end, 8):
            rest = end - j - 8
            tops = {k: m_ref[j : j + 8, k * lanes : (k + 1) * lanes] for k in live}
            tails = {k: m_ref[j + 8 : end, k * lanes : (k + 1) * lanes] for k in live} if rest else {}
            kd, off = j // lanes, j % lanes
            cols = []
            for c in range(8):
                top = jnp.broadcast_to(tops[kd][:, off + c : off + c + 1], (8, lanes))
                tail = jnp.broadcast_to(tails[kd][:, off + c : off + c + 1], (rest, lanes)) if rest else None
                cols.append((top, tail))
            for c in range(8):
                top, tail = cols[c]
                inv = lax.rsqrt(top[c : c + 1, :])
                top = top * inv
                if rest:
                    tail = tail * inv
                for k in range(c + 1, 8):
                    scale = top[k : k + 1, :]
                    tk, lk = cols[k]
                    cols[k] = (tk - top * scale, lk - tail * scale if rest else None)
                for k in live:
                    row = tops[k][c : c + 1, :] * inv
                    tops[k] = jnp.where(sub == c, row, jnp.where(sub > c, tops[k] - top * row, tops[k]))
                    if rest:
                        tails[k] = tails[k] - tail * row
            for k in live:
                m_ref[j : j + 8, k * lanes : (k + 1) * lanes] = tops[k]
                if rest:
                    m_ref[j + 8 : end, k * lanes : (k + 1) * lanes] = tails[k]
        if end < n:
            first, last = live[0] * lanes, (live[-1] + 1) * lanes
            base = (end // lanes) * lanes
            update = lax.dot_general(
                m_ref[o:end, base:n], m_ref[o:end, first:last], TN,
                precision=lax.Precision.HIGHEST, preferred_element_type=F32,
            )
            m_ref[end:n, first:last] = m_ref[end:n, first:last] - update[end - base :, :]
    out_ref[...] = jnp.where(ri >= ci, m_ref[:, n:], 0.0)


def factor_inverse(gram, other):
    n = gram.shape[0]
    return pl.pallas_call(
        functools.partial(factor_kernel, n=n, outer=64),
        out_shape=jax.ShapeDtypeStruct((n, n), F32),
        scratch_shapes=[pltpu.VMEM((n, 2 * n), F32)],
        cost_estimate=cost(9),
        name="factor_inverse",
    )(gram, other)


def right_kernel(inv_ref, w_ref, other_ref, right_ref, pair_ref, inv_pair_ref, square_ref):
    inverse = inv_ref[...]
    rank = inverse.shape[0]
    right = dot3(split(inverse), split(w_ref[...] + other_ref[...]), MM)
    pair_ref[:rank, :], pair_ref[rank:, :] = split(right)
    inv_pair_ref[:rank, :], inv_pair_ref[rank:, :] = split(inverse.T)
    right = right.T
    right_ref[...] = right
    square_ref[...] = jnp.sum(right * right, axis=0, keepdims=True)


def right_part(inverse, weight, other):
    rank, cols = weight.shape
    return pl.pallas_call(
        right_kernel,
        out_shape=[
            jax.ShapeDtypeStruct((cols, rank), F32),
            jax.ShapeDtypeStruct((2 * rank, cols), BF16),
            jax.ShapeDtypeStruct((2 * rank, rank), BF16),
            jax.ShapeDtypeStruct((1, rank), F32),
        ],
        cost_estimate=cost(3),
        name="right_part",
    )(inverse, weight, other)


def momentum_kernel(m_ref, g_ref, left_ref, inv_ref, right_ref, *rest):
    out_ref, orth_ref = rest[-2:]
    rank = inv_ref.shape[1]
    orth = dot3(split(left_ref[...]), (inv_ref[:rank, :], inv_ref[rank:, :]), MM)
    orth_ref[...] = orth
    feedback = lax.dot_general(orth.astype(BF16), right_ref[...], MM, preferred_element_type=F32)
    out_ref[...] = m_ref[...] + g_ref[...].astype(F32) - FEEDBACK * feedback


def momentum_rows(momentum, gradient, left, inv_pair, pair, start, count, block, carry):
    rows, cols = momentum.shape
    rank = left.shape[1]
    row = lambda i: (start + i, 0)
    whole = lambda i: (0, 0)
    return pl.pallas_call(
        momentum_kernel,
        grid=(count,),
        in_specs=[
            pl.BlockSpec((block, cols), row),
            pl.BlockSpec((block, cols), row),
            pl.BlockSpec((block, rank), row),
            pl.BlockSpec((2 * rank, rank), whole),
            pl.BlockSpec((rank, cols), whole),
        ]
        + [pl.BlockSpec(memory_space=pl.ANY)] * len(carry),
        out_specs=[pl.BlockSpec((block, cols), row), pl.BlockSpec((block, rank), row)],
        out_shape=[jax.ShapeDtypeStruct((rows, cols), F32), jax.ShapeDtypeStruct((rows, rank), F32)],
        input_output_aliases={5 + k: k for k in range(len(carry))},
        cost_estimate=cost(4),
        name="momentum_rows",
    )(momentum, gradient, left, inv_pair, pair, *carry)


def update_kernel(core_ref, orth_ref, pair_ref, square_ref, share_ref, out_ref, next_ref, *, factor):
    norm = jnp.sqrt(square_ref[...] + EPS)
    rank = orth_ref.shape[1]

    @pl.when(pl.program_id(0) == 0)
    def _():
        next_ref[...] = share_ref[...] / norm

    orth = orth_ref[...] * (factor / norm)
    out_ref[...] = dot3(split(orth), (pair_ref[:rank, :], pair_ref[rank:, :]), MM).astype(BF16)


def update_rows(orth, pair, squares, right, core, share, factor, block):
    rows, rank = orth.shape
    cols = pair.shape[1]
    whole = lambda i, s: (0, 0)
    return pl.pallas_call(
        functools.partial(update_kernel, factor=factor),
        grid_spec=pltpu.PrefetchScalarGridSpec(
            num_scalar_prefetch=1,
            grid=(rows // block,),
            in_specs=[
                pl.BlockSpec((block, rank), lambda i, s: (i, 0)),
                pl.BlockSpec(pair.shape, whole),
                pl.BlockSpec(squares.shape, whole),
                pl.BlockSpec((share, rank), lambda i, s: (s[0], 0)),
            ],
            out_specs=[pl.BlockSpec((block, cols), lambda i, s: (i, 0)), pl.BlockSpec((share, rank), whole)],
        ),
        out_shape=[jax.ShapeDtypeStruct((rows, cols), BF16), jax.ShapeDtypeStruct((share, rank), F32)],
        cost_estimate=cost(5),
        name="update_rows",
    )(core.reshape(1).astype(jnp.int32), orth, pair, squares, right)


def swap(x, axis, size, step):
    return lax.ppermute(x, axis, [(i, i ^ step) for i in range(size)])


def row_rest(x, size):
    if size == 1:
        return jnp.zeros_like(x)
    total, step = swap(x, "row", size, 1), 2
    while step < size:
        whole = x + total
        total = total + swap(whole, "row", size, step)
        step *= 2
    return total


def groups_of(size):
    bits = size.bit_length() - 1
    groups, low = [], 2
    while low < bits:
        width = min(2, bits - low)
        groups.append((1 << low, 1 << width))
        low += width
    return groups


def scatter_sum(x, position, size):
    for step, members in groups_of(size):
        mine = (position // step) % members
        rows = x.shape[0] // members
        part = lambda k: lax.dynamic_slice_in_dim(x, k * rows, rows)
        got = [swap(part(mine ^ d), "col", size, d * step) for d in range(1, members)]
        x = part(mine)
        for piece in got:
            x = x + piece
    return x


def gather_rows(x, position, size):
    for step, members in reversed(groups_of(size)):
        mine = (position // step) % members
        pieces = [x] + [swap(x, "col", size, d * step) for d in range(1, members)]
        width = 1
        while width < members:
            odd = (mine // width) % 2 == 1
            pieces = [
                jnp.where(odd, jnp.concatenate([b, a]), jnp.concatenate([a, b]))
                for a, b in zip(pieces[0::2], pieces[1::2])
            ]
            width *= 2
        x = pieces[0]
    return x


def body(gradient, momentum, right_factor, *, cols_size, rows_size, factor):
    rows, cols = momentum.shape
    block = rows // 8
    half, quarter = rows // 2, rows // 4
    position = lax.axis_index("col")
    x, y = position % 2, (position // 2) % 2
    core = lax.axis_index("row")
    if rows_size == 2:
        rest = swap(right_factor, "row", 2, 1)
    else:
        rest = lax.all_gather(right_factor, "row", axis=0, tiled=True)

    pieces = lambda a, b: left_rows(
        momentum, gradient, right_factor, rest, core, cols, (a * quarter, half + b * quarter), quarter, block
    )
    send_a, send_b = pieces(1 - x, 1 - y)
    got_a = swap(send_a, "col", cols_size, 1)
    got_b = swap(send_b, "col", cols_size, 2)
    keep_a, keep_b = pieces(x, y)

    def part(a, b, k):
        return lax.dynamic_slice_in_dim(a, k * block, block) + lax.dynamic_slice_in_dim(b, k * block, block)

    next_a = swap(part(keep_a, got_a, 1 - y), "col", cols_size, 2)
    next_b = swap(part(keep_b, got_b, 1 - x), "col", cols_size, 1)
    own_a = part(keep_a, got_a, y) + next_a
    own_b = part(keep_b, got_b, x) + next_b
    own = jnp.concatenate([own_a.reshape(-1, block // (cols_size // 4), own_a.shape[1]),
                           own_b.reshape(-1, block // (cols_size // 4), own_b.shape[1])], axis=1)
    own = scatter_sum(own, position, cols_size)

    near = gather_rows(own, position, cols_size)
    cut = block // (cols_size // 4)
    near_a = near[:, :cut].reshape(block, -1)
    near_b = near[:, cut:].reshape(block, -1)
    side_a = swap(near_a, "col", cols_size, 2)
    side_b = swap(near_b, "col", cols_size, 1)
    pair_a = jnp.where(y == 1, jnp.concatenate([side_a, near_a]), jnp.concatenate([near_a, side_a]))
    pair_b = jnp.where(x == 1, jnp.concatenate([side_b, near_b]), jnp.concatenate([near_b, side_b]))
    far_a = swap(pair_a, "col", cols_size, 1)
    far_b = swap(pair_b, "col", cols_size, 2)
    carry = weight_rows(momentum, gradient, near_a, near_b,
                        (x * quarter + y * block, half + y * quarter + x * block), block)
    carry = weight_rows(momentum, gradient, side_a, side_b,
                        (x * quarter + (1 - y) * block, half + y * quarter + (1 - x) * block), block, carry)
    weight, gram, left = weight_rows(momentum, gradient, far_a, far_b,
                                     ((1 - x) * quarter, half + (1 - y) * quarter), block, carry)

    gram_rest = row_rest(gram, rows_size)
    weight_rest = row_rest(weight, rows_size)
    inverse = factor_inverse(gram, gram_rest)
    right, pair, inv_pair, squares = right_part(inverse, weight, weight_rest)
    steps = cols_size.bit_length() - 1
    chunk = max(1, 8 // steps)
    carry, start = (), 0
    for k in range(steps):
        got = swap(squares, "col", cols_size, 1 << k)
        count = chunk if k + 1 < steps else 8 - start
        carry = momentum_rows(momentum, gradient, left, inv_pair, pair, start, count, block, carry)
        start += count
        got, *carry = lax.optimization_barrier((got, *carry))
        squares = squares + got
    momentum_next, orth = carry
    update, right_next = update_rows(orth, pair, squares, right, core, cols // rows_size, factor, block)
    return (momentum_next, right_next, update)


def solution(mesh):
    cols_size, rows_size = mesh.shape["col"], mesh.shape["row"]

    def step(gradient, momentum, right_factor):
        rows, cols = momentum.shape
        factor = math.sqrt(rows * cols / right_factor.shape[1])
        placed = (P("row", "col"), P("row", "col"), P(("col", "row"), None))
        return jax.shard_map(
            functools.partial(body, cols_size=cols_size, rows_size=rows_size, factor=factor),
            mesh=mesh,
            in_specs=placed,
            out_specs=(P("row", "col"), P(("col", "row"), None), P("row", "col")),
            check_vma=False,
        )(gradient, momentum, right_factor)

    return step
```

```python
import functools
import math

import jax
import jax.numpy as jnp
from jax import lax
from jax.experimental import pallas as pl
from jax.experimental.pallas import tpu as pltpu
from jax.sharding import PartitionSpec as P

EPS = 1e-06
FEEDBACK = 0.05
F32 = jnp.float32
BF16 = jnp.bfloat16


MM = (((1,), (0,)), ((), ()))
TN = (((0,), (0,)), ((), ()))
NT = (((1,), (1,)), ((), ()))


def split(x):
    high = x.astype(BF16)
    return high, (x - high.astype(F32)).astype(BF16)


def dot3(a, b, dims):
    (da,), (db,) = dims[0]
    left = jnp.concatenate([a[0], a[1], a[0]], axis=da)
    right = jnp.concatenate([b[0], b[0], b[1]], axis=db)
    return lax.dot_general(left, right, dims, preferred_element_type=F32)


def params(mib):
    return pltpu.CompilerParams(vmem_limit_bytes=mib << 20)


def cost(us):
    return pl.CostEstimate(flops=int(us * 1e9), bytes_accessed=1 << 20, transcendentals=0)


def left_kernel(at_ref, m_ref, g_ref, own_ref, rest_ref, a_ref, b_ref, high_ref, low_ref, *, block, half):
    i = pl.program_id(0)

    @pl.when(i == 0)
    def _():
        own, share = at_ref[1], own_ref.shape[0]
        for k in range(high_ref.shape[0] // share):
            rows = pl.ds(k * share, share)

            @pl.when(own == k)
            def _():
                high_ref[rows, :], low_ref[rows, :] = split(own_ref[...])

            @pl.when(own != k)
            def _():
                high_ref[rows, :], low_ref[rows, :] = split(rest_ref[rest_rows(rest_ref, share, k), :])

    blend = split(m_ref[...] + g_ref[...].astype(F32))
    out = dot3(blend, (high_ref[...], low_ref[...]), MM)

    @pl.when(i < half)
    def _():
        a_ref[pl.ds(pl.multiple_of(i * block, block), block), :] = out

    @pl.when(i >= half)
    def _():
        b_ref[pl.ds(pl.multiple_of((i - half) * block, block), block), :] = out


def rest_rows(rest_ref, share, k):
    return pl.ds(0 if rest_ref.shape[0] == share else k * share, share)


def block_map(starts, half, block):
    def at(i, s):
        a, b = starts(s[0] % 2, (s[0] // 2) % 2)
        return jnp.where(i < half, a // block + i, b // block + i - half), 0

    return at


def left_rows(where, momentum, gradient, own, rest, cols, starts, rows):
    rank = own.shape[1]
    block = rows
    half = rows // block
    at = block_map(starts, half, block)
    whole = lambda i, s: (0, 0)
    return pl.pallas_call(
        functools.partial(left_kernel, block=block, half=half),
        grid_spec=pltpu.PrefetchScalarGridSpec(
            num_scalar_prefetch=1,
            grid=(2 * half,),
            in_specs=[
                pl.BlockSpec((block, cols), at),
                pl.BlockSpec((block, cols), at),
                pl.BlockSpec(own.shape, whole),
                pl.BlockSpec(rest.shape, whole),
            ],
            out_specs=[pl.BlockSpec((rows, rank), whole), pl.BlockSpec((rows, rank), whole)],
            scratch_shapes=[pltpu.VMEM((cols, rank), BF16), pltpu.VMEM((cols, rank), BF16)],
        ),
        out_shape=[jax.ShapeDtypeStruct((rows, rank), F32), jax.ShapeDtypeStruct((rows, rank), F32)],
        cost_estimate=cost(5),
        compiler_params=params(58),
        name="left_rows",
    )(where, momentum, gradient, own, rest)


def weight_kernel(at_ref, m_ref, g_ref, a_ref, b_ref, *rest, block, half, first):
    if first:
        w_ref, gram_ref, left_ref = rest
    else:
        w_in, gram_in, _, w_ref, gram_ref, left_ref = rest
    i = pl.program_id(0)

    @pl.when(i == 0)
    def _():
        if first:
            w_ref[...] = jnp.zeros_like(w_ref)
            gram_ref[...] = jnp.zeros_like(gram_ref)
        else:
            w_ref[...] = w_in[...]
            gram_ref[...] = gram_in[...]

    @pl.when(i < half)
    def _():
        left_ref[...] = a_ref[pl.ds(pl.multiple_of(i * block, block), block), :]

    @pl.when(i >= half)
    def _():
        left_ref[...] = b_ref[pl.ds(pl.multiple_of((i - half) * block, block), block), :]

    left = split(left_ref[...])
    blend = split(m_ref[...] + g_ref[...].astype(F32))
    w_ref[...] += dot3(left, blend, TN)
    gram_ref[...] += dot3(left, left, TN)


def weight_rows(where, momentum, gradient, piece_a, piece_b, starts, carry=None):
    all_rows, cols = momentum.shape
    rows, rank = piece_a.shape
    block = rows
    half = rows // block
    blocks = 2 * half
    at = block_map(starts, half, block)
    whole = lambda i, s: (0, 0)
    in_specs = [
        pl.BlockSpec((block, cols), at),
        pl.BlockSpec((block, cols), at),
        pl.BlockSpec((rows, rank), whole),
        pl.BlockSpec((rows, rank), whole),
    ]
    args = [momentum, gradient, piece_a, piece_b]
    aliases = {}
    if carry is not None:
        in_specs += [
            pl.BlockSpec((rank, cols), whole),
            pl.BlockSpec((rank, rank), whole),
            pl.BlockSpec(memory_space=pl.ANY),
        ]
        args += list(carry)
        aliases = {7: 2}
    return pl.pallas_call(
        functools.partial(weight_kernel, block=block, half=half, first=carry is None),
        grid_spec=pltpu.PrefetchScalarGridSpec(
            num_scalar_prefetch=1,
            grid=(blocks,),
            in_specs=in_specs,
            out_specs=[
                pl.BlockSpec((rank, cols), whole),
                pl.BlockSpec((rank, rank), whole),
                pl.BlockSpec((block, rank), at),
            ],
        ),
        out_shape=[
            jax.ShapeDtypeStruct((rank, cols), F32),
            jax.ShapeDtypeStruct((rank, rank), F32),
            jax.ShapeDtypeStruct((all_rows, rank), F32),
        ],
        input_output_aliases=aliases,
        cost_estimate=cost(2),
        compiler_params=params(30),
        name="weight_rows",
    )(where, *args)


def factor_kernel(gram_ref, other_ref, out_ref, m_ref, *, n, outer):
    lanes = 128
    chunks = n // lanes
    m_ref[:, :n] = gram_ref[...] + other_ref[...]
    ri = lax.broadcasted_iota(jnp.int32, (n, n), 0)
    ci = lax.broadcasted_iota(jnp.int32, (n, n), 1)
    m_ref[:, n:] = jnp.where(ri == ci, 1.0, 0.0).astype(F32)
    sub = lax.broadcasted_iota(jnp.int32, (8, lanes), 0)
    for o in range(0, n, outer):
        end = o + outer
        live = [k for k in range(chunks) if (k + 1) * lanes > o]
        live += [k + chunks for k in range(chunks) if k * lanes < end]
        for j in range(o, end, 8):
            rest = end - j - 8
            tops = {k: m_ref[j : j + 8, k * lanes : (k + 1) * lanes] for k in live}
            tails = {k: m_ref[j + 8 : end, k * lanes : (k + 1) * lanes] for k in live} if rest else {}
            kd, off = j // lanes, j % lanes
            cols = []
            for c in range(8):
                top = jnp.broadcast_to(tops[kd][:, off + c : off + c + 1], (8, lanes))
                tail = jnp.broadcast_to(tails[kd][:, off + c : off + c + 1], (rest, lanes)) if rest else None
                cols.append((top, tail))
            for c in range(8):
                top, tail = cols[c]
                inv = lax.rsqrt(top[c : c + 1, :])
                top = top * inv
                if rest:
                    tail = tail * inv
                for k in range(c + 1, 8):
                    scale = top[k : k + 1, :]
                    tk, lk = cols[k]
                    cols[k] = (tk - top * scale, lk - tail * scale if rest else None)
                for k in live:
                    row = tops[k][c : c + 1, :] * inv
                    tops[k] = jnp.where(sub == c, row, jnp.where(sub > c, tops[k] - top * row, tops[k]))
                    if rest:
                        tails[k] = tails[k] - tail * row
            for k in live:
                m_ref[j : j + 8, k * lanes : (k + 1) * lanes] = tops[k]
                if rest:
                    m_ref[j + 8 : end, k * lanes : (k + 1) * lanes] = tails[k]
        if end < n:
            first, last = live[0] * lanes, (live[-1] + 1) * lanes
            base = (end // lanes) * lanes
            update = lax.dot_general(
                m_ref[o:end, base:n], m_ref[o:end, first:last], TN,
                precision=lax.Precision.HIGHEST, preferred_element_type=F32,
            )
            m_ref[end:n, first:last] = m_ref[end:n, first:last] - update[end - base :, :]
    out_ref[...] = jnp.where(ri >= ci, m_ref[:, n:], 0.0)


def factor_inverse(gram, other):
    n = gram.shape[0]
    return pl.pallas_call(
        functools.partial(factor_kernel, n=n, outer=64),
        out_shape=jax.ShapeDtypeStruct((n, n), F32),
        scratch_shapes=[pltpu.VMEM((n, 2 * n), F32)],
        cost_estimate=cost(9),
        compiler_params=params(6),
        name="factor_inverse",
    )(gram, other)


def right_kernel(inv_ref, w_ref, other_ref, right_ref, pair_ref, inv_pair_ref, square_ref):
    inverse = inv_ref[...]
    rank = inverse.shape[0]
    right = dot3(split(inverse), split(w_ref[...] + other_ref[...]), MM)
    pair_ref[:rank, :], pair_ref[rank:, :] = split(right)
    inv_pair_ref[:rank, :], inv_pair_ref[rank:, :] = split(inverse.T)
    right = right.T
    right_ref[...] = right
    square_ref[...] = jnp.sum(right * right, axis=0, keepdims=True)


def right_part(inverse, weight, other):
    rank, cols = weight.shape
    return pl.pallas_call(
        right_kernel,
        out_shape=[
            jax.ShapeDtypeStruct((cols, rank), F32),
            jax.ShapeDtypeStruct((2 * rank, cols), BF16),
            jax.ShapeDtypeStruct((2 * rank, rank), BF16),
            jax.ShapeDtypeStruct((1, rank), F32),
        ],
        cost_estimate=cost(3),
        compiler_params=params(16),
        name="right_part",
    )(inverse, weight, other)


def momentum_kernel(m_ref, g_ref, left_ref, inv_ref, right_ref, *rest):
    out_ref, orth_ref = rest[-2:]
    rank = inv_ref.shape[1]
    orth = dot3(split(left_ref[...]), (inv_ref[:rank, :], inv_ref[rank:, :]), MM)
    orth_ref[...] = orth
    feedback = lax.dot_general(orth.astype(BF16), right_ref[...], MM, preferred_element_type=F32)
    out_ref[...] = m_ref[...] + g_ref[...].astype(F32) - FEEDBACK * feedback


def momentum_rows(momentum, gradient, left, inv_pair, pair, start, count, block, carry):
    rows, cols = momentum.shape
    rank = left.shape[1]
    row = lambda i: (start + i, 0)
    whole = lambda i: (0, 0)
    return pl.pallas_call(
        momentum_kernel,
        grid=(count,),
        in_specs=[
            pl.BlockSpec((block, cols), row),
            pl.BlockSpec((block, cols), row),
            pl.BlockSpec((block, rank), row),
            pl.BlockSpec((2 * rank, rank), whole),
            pl.BlockSpec((rank, cols), whole),
        ]
        + [pl.BlockSpec(memory_space=pl.ANY)] * len(carry),
        out_specs=[pl.BlockSpec((block, cols), row), pl.BlockSpec((block, rank), row)],
        out_shape=[jax.ShapeDtypeStruct((rows, cols), F32), jax.ShapeDtypeStruct((rows, rank), F32)],
        input_output_aliases={5 + k: k for k in range(len(carry))},
        cost_estimate=cost(4),
        compiler_params=params(20),
        name="momentum_rows",
    )(momentum, gradient, left, inv_pair, pair, *carry)


def update_kernel(core_ref, orth_ref, pair_ref, square_ref, share_ref, out_ref, next_ref, *, factor):
    norm = jnp.sqrt(square_ref[...] + EPS)
    rank = orth_ref.shape[1]

    @pl.when(pl.program_id(0) == 0)
    def _():
        next_ref[...] = share_ref[...] / norm

    orth = orth_ref[...] * (factor / norm)
    out_ref[...] = dot3(split(orth), (pair_ref[:rank, :], pair_ref[rank:, :]), MM).astype(BF16)


def update_rows(where, orth, pair, squares, right, share, factor, block):
    rows, rank = orth.shape
    cols = pair.shape[1]
    whole = lambda i, s: (0, 0)
    return pl.pallas_call(
        functools.partial(update_kernel, factor=factor),
        grid_spec=pltpu.PrefetchScalarGridSpec(
            num_scalar_prefetch=1,
            grid=(rows // block,),
            in_specs=[
                pl.BlockSpec((block, rank), lambda i, s: (i, 0)),
                pl.BlockSpec(pair.shape, whole),
                pl.BlockSpec(squares.shape, whole),
                pl.BlockSpec((share, rank), lambda i, s: (s[1], 0)),
            ],
            out_specs=[pl.BlockSpec((block, cols), lambda i, s: (i, 0)), pl.BlockSpec((share, rank), whole)],
        ),
        out_shape=[jax.ShapeDtypeStruct((rows, cols), BF16), jax.ShapeDtypeStruct((share, rank), F32)],
        cost_estimate=cost(5),
        compiler_params=params(20),
        name="update_rows",
    )(where, orth, pair, squares, right)


def swap(x, axis, size, step):
    return lax.ppermute(x, axis, [(i, i ^ step) for i in range(size)])


def row_rest(x, size):
    if size == 1:
        return jnp.zeros_like(x)
    total, step = swap(x, "row", size, 1), 2
    while step < size:
        whole = x + total
        total = total + swap(whole, "row", size, step)
        step *= 2
    return total


def groups_of(size):
    bits = size.bit_length() - 1
    groups, low = [], 2
    while low < bits:
        width = min(2, bits - low)
        groups.append((1 << low, 1 << width))
        low += width
    return groups


def scatter_sum(x, position, size):
    for step, members in groups_of(size):
        mine = (position // step) % members
        rows = x.shape[0] // members
        part = lambda k: lax.dynamic_slice_in_dim(x, k * rows, rows)
        got = [swap(part(mine ^ d), "col", size, d * step) for d in range(1, members)]
        x = part(mine)
        for piece in got:
            x = x + piece
    return x


def gather_rows(x, position, size):
    for step, members in reversed(groups_of(size)):
        mine = (position // step) % members
        pieces = [x] + [swap(x, "col", size, d * step) for d in range(1, members)]
        width = 1
        while width < members:
            odd = (mine // width) % 2 == 1
            pieces = [
                jnp.where(odd, jnp.concatenate([b, a]), jnp.concatenate([a, b]))
                for a, b in zip(pieces[0::2], pieces[1::2])
            ]
            width *= 2
        x = pieces[0]
    return x


def body(gradient, momentum, right_factor, *, cols_size, rows_size, factor):
    rows, cols = momentum.shape
    block = rows // 8
    half, quarter = rows // 2, rows // 4
    position = lax.axis_index("col")
    x, y = position % 2, (position // 2) % 2
    where = jnp.stack([position, lax.axis_index("row")]).astype(jnp.int32)
    if rows_size == 2:
        rest = swap(right_factor, "row", 2, 1)
    else:
        rest = lax.all_gather(right_factor, "row", axis=0, tiled=True)

    pieces = lambda starts: left_rows(where, momentum, gradient, right_factor, rest, cols, starts, quarter)
    send_a, send_b = pieces(lambda x, y: ((1 - x) * quarter, half + (1 - y) * quarter))
    got_a = swap(send_a, "col", cols_size, 1)
    got_b = swap(send_b, "col", cols_size, 2)
    keep_a, keep_b = pieces(lambda x, y: (x * quarter, half + y * quarter))

    def part(a, b, k):
        return lax.dynamic_slice_in_dim(a, k * block, block) + lax.dynamic_slice_in_dim(b, k * block, block)

    next_a = swap(part(keep_a, got_a, 1 - y), "col", cols_size, 2)
    next_b = swap(part(keep_b, got_b, 1 - x), "col", cols_size, 1)
    own_a = part(keep_a, got_a, y) + next_a
    own_b = part(keep_b, got_b, x) + next_b
    own = jnp.concatenate([own_a.reshape(-1, block // (cols_size // 4), own_a.shape[1]),
                           own_b.reshape(-1, block // (cols_size // 4), own_b.shape[1])], axis=1)
    own = scatter_sum(own, position, cols_size)

    near = gather_rows(own, position, cols_size)
    cut = block // (cols_size // 4)
    near_a = near[:, :cut].reshape(block, -1)
    near_b = near[:, cut:].reshape(block, -1)
    side_a = swap(near_a, "col", cols_size, 2)
    side_b = swap(near_b, "col", cols_size, 1)
    pair_a = jnp.where(y == 1, jnp.concatenate([side_a, near_a]), jnp.concatenate([near_a, side_a]))
    pair_b = jnp.where(x == 1, jnp.concatenate([side_b, near_b]), jnp.concatenate([near_b, side_b]))
    far_a = swap(pair_a, "col", cols_size, 1)
    far_b = swap(pair_b, "col", cols_size, 2)
    weigh = functools.partial(weight_rows, where, momentum, gradient)
    carry = weigh(near_a, near_b, lambda x, y: (x * quarter + y * block, half + y * quarter + x * block))
    carry = weigh(
        side_a, side_b, lambda x, y: (x * quarter + (1 - y) * block, half + y * quarter + (1 - x) * block), carry
    )
    weight, gram, left = weigh(far_a, far_b, lambda x, y: ((1 - x) * quarter, half + (1 - y) * quarter), carry)

    gram_rest = row_rest(gram, rows_size)
    weight_rest = row_rest(weight, rows_size)
    inverse = factor_inverse(gram, gram_rest)
    right, pair, inv_pair, squares = right_part(inverse, weight, weight_rest)
    steps = cols_size.bit_length() - 1
    chunk = max(1, 8 // steps)
    carry, start = (), 0
    for k in range(steps):
        got = swap(squares, "col", cols_size, 1 << k)
        count = chunk if k + 1 < steps else 8 - start
        carry = momentum_rows(momentum, gradient, left, inv_pair, pair, start, count, block, carry)
        start += count
        got, *carry = lax.optimization_barrier((got, *carry))
        squares = squares + got
    momentum_next, orth = carry
    update, right_next = update_rows(where, orth, pair, squares, right, cols // rows_size, factor, 2 * block)
    return (momentum_next, right_next, update)


def solution(mesh):
    cols_size, rows_size = mesh.shape["col"], mesh.shape["row"]

    def step(gradient, momentum, right_factor):
        rows, cols = momentum.shape
        factor = math.sqrt(rows * cols / right_factor.shape[1])
        placed = (P("row", "col"), P("row", "col"), P(("col", "row"), None))
        return jax.shard_map(
            functools.partial(body, cols_size=cols_size, rows_size=rows_size, factor=factor),
            mesh=mesh,
            in_specs=placed,
            out_specs=(P("row", "col"), P(("col", "row"), None), P("row", "col")),
            check_vma=False,
        )(gradient, momentum, right_factor)

    return step
```

```python
import functools
import math

import jax
import jax.numpy as jnp
from jax import lax
from jax.experimental import pallas as pl
from jax.experimental.pallas import tpu as pltpu
from jax.sharding import PartitionSpec as P

EPS = 1e-06
FEEDBACK = 0.05
F32 = jnp.float32
BF16 = jnp.bfloat16


MM = (((1,), (0,)), ((), ()))
TN = (((0,), (0,)), ((), ()))
NT = (((1,), (1,)), ((), ()))


def split(x):
    high = x.astype(BF16)
    return high, (x - high.astype(F32)).astype(BF16)


def dot3(a, b, dims):
    (da,), (db,) = dims[0]
    left = jnp.concatenate([a[0], a[1], a[0]], axis=da)
    right = jnp.concatenate([b[0], b[0], b[1]], axis=db)
    return lax.dot_general(left, right, dims, preferred_element_type=F32)


def params(mib):
    return pltpu.CompilerParams(vmem_limit_bytes=mib << 20)


def cost(us):
    return pl.CostEstimate(flops=int(us * 1e9), bytes_accessed=1 << 20, transcendentals=0)


def left_kernel(
    where_ref, m_ref, g_ref, own_ref, rest_ref, a_ref, b_ref, m_buf, g_buf, own_buf, high_ref, low_ref, sems, *, starts, block
):
    position, own = where_ref[0], where_ref[1]
    copies = []
    for k, start in enumerate(starts(position % 2, (position // 2) % 2)):
        rows = pl.ds(pl.multiple_of(start, block), block)
        copies.append(
            (
                pltpu.make_async_copy(m_ref.at[rows], m_buf.at[k], sems.at[k, 0]),
                pltpu.make_async_copy(g_ref.at[rows], g_buf.at[k], sems.at[k, 1]),
            )
        )
    own_copy = pltpu.make_async_copy(own_ref, own_buf, sems.at[2, 0])
    own_copy.start()
    for pair in copies:
        for copy in pair:
            copy.start()
    own_copy.wait()

    share = own_ref.shape[0]
    for k in range(high_ref.shape[0] // share):
        rows = pl.ds(k * share, share)

        @pl.when(own == k)
        def _():
            high_ref[rows, :], low_ref[rows, :] = split(own_buf[...])

        @pl.when(own != k)
        def _():
            high_ref[rows, :], low_ref[rows, :] = split(rest_ref[rest_rows(rest_ref, share, k), :])

    for k, out_ref in enumerate((a_ref, b_ref)):
        for copy in copies[k]:
            copy.wait()
        blend = split(m_buf[k] + g_buf[k].astype(F32))
        out_ref[...] = dot3(blend, (high_ref[...], low_ref[...]), MM)


def rest_rows(rest_ref, share, k):
    return pl.ds(0 if rest_ref.shape[0] == share else k * share, share)


def block_map(starts, half, block):
    def at(i, s):
        a, b = starts(s[0] % 2, (s[0] // 2) % 2)
        return jnp.where(i < half, a // block + i, b // block + i - half), 0

    return at


def left_rows(where, momentum, gradient, own, rest, cols, block, starts):
    rank = own.shape[1]
    vmem, hbm = pl.BlockSpec(memory_space=pltpu.VMEM), pl.BlockSpec(memory_space=pltpu.HBM)
    return pl.pallas_call(
        functools.partial(left_kernel, starts=starts, block=block),
        in_specs=[pl.BlockSpec(memory_space=pltpu.SMEM), hbm, hbm, hbm, vmem],
        out_specs=[vmem, vmem],
        scratch_shapes=[
            pltpu.VMEM((2, block, cols), F32),
            pltpu.VMEM((2, block, cols), BF16),
            pltpu.VMEM(own.shape, F32),
            pltpu.VMEM((cols, rank), BF16),
            pltpu.VMEM((cols, rank), BF16),
            pltpu.SemaphoreType.DMA((3, 2)),
        ],
        out_shape=[jax.ShapeDtypeStruct((block, rank), F32), jax.ShapeDtypeStruct((block, rank), F32)],
        cost_estimate=cost(3),
        compiler_params=params(16),
        name="left_rows",
    )(where, *(pltpu.with_memory_space_constraint(v, pltpu.HBM) for v in (momentum, gradient, own)), rest)


def weight_kernel(at_ref, m_ref, g_ref, a_ref, b_ref, *rest, block, half, first):
    if first:
        w_ref, gram_ref, left_ref = rest
    else:
        w_in, gram_in, _, w_ref, gram_ref, left_ref = rest
    i = pl.program_id(0)

    @pl.when(i == 0)
    def _():
        if first:
            w_ref[...] = jnp.zeros_like(w_ref)
            gram_ref[...] = jnp.zeros_like(gram_ref)
        else:
            w_ref[...] = w_in[...]
            gram_ref[...] = gram_in[...]

    @pl.when(i < half)
    def _():
        left_ref[...] = a_ref[pl.ds(pl.multiple_of(i * block, block), block), :]

    @pl.when(i >= half)
    def _():
        left_ref[...] = b_ref[pl.ds(pl.multiple_of((i - half) * block, block), block), :]

    left = split(left_ref[...])
    blend = split(m_ref[...] + g_ref[...].astype(F32))
    w_ref[...] += dot3(left, blend, TN)
    gram_ref[...] += dot3(left, left, TN)


def weight_rows(where, momentum, gradient, piece_a, piece_b, starts, carry=None):
    all_rows, cols = momentum.shape
    rows, rank = piece_a.shape
    block = rows
    half = rows // block
    blocks = 2 * half
    at = block_map(starts, half, block)
    whole = lambda i, s: (0, 0)
    in_specs = [
        pl.BlockSpec((block, cols), at),
        pl.BlockSpec((block, cols), at),
        pl.BlockSpec((rows, rank), whole),
        pl.BlockSpec((rows, rank), whole),
    ]
    args = [momentum, gradient, piece_a, piece_b]
    aliases = {}
    if carry is not None:
        in_specs += [
            pl.BlockSpec((rank, cols), whole),
            pl.BlockSpec((rank, rank), whole),
            pl.BlockSpec(memory_space=pl.ANY),
        ]
        args += list(carry)
        aliases = {7: 2}
    return pl.pallas_call(
        functools.partial(weight_kernel, block=block, half=half, first=carry is None),
        grid_spec=pltpu.PrefetchScalarGridSpec(
            num_scalar_prefetch=1,
            grid=(blocks,),
            in_specs=in_specs,
            out_specs=[
                pl.BlockSpec((rank, cols), whole),
                pl.BlockSpec((rank, rank), whole),
                pl.BlockSpec((block, rank), at),
            ],
        ),
        out_shape=[
            jax.ShapeDtypeStruct((rank, cols), F32),
            jax.ShapeDtypeStruct((rank, rank), F32),
            jax.ShapeDtypeStruct((all_rows, rank), F32),
        ],
        input_output_aliases=aliases,
        cost_estimate=cost(2),
        compiler_params=params(30),
        name="weight_rows",
    )(where, *args)


def factor_kernel(gram_ref, other_ref, out_ref, m_ref, *, n, outer):
    lanes = 128
    chunks = n // lanes
    m_ref[:, :n] = gram_ref[...] + other_ref[...]
    ri = lax.broadcasted_iota(jnp.int32, (n, n), 0)
    ci = lax.broadcasted_iota(jnp.int32, (n, n), 1)
    m_ref[:, n:] = jnp.where(ri == ci, 1.0, 0.0).astype(F32)
    sub = lax.broadcasted_iota(jnp.int32, (8, lanes), 0)
    for o in range(0, n, outer):
        end = o + outer
        live = [k for k in range(chunks) if (k + 1) * lanes > o]
        live += [k + chunks for k in range(chunks) if k * lanes < end]
        for j in range(o, end, 8):
            rest = end - j - 8
            tops = {k: m_ref[j : j + 8, k * lanes : (k + 1) * lanes] for k in live}
            tails = {k: m_ref[j + 8 : end, k * lanes : (k + 1) * lanes] for k in live} if rest else {}
            kd, off = j // lanes, j % lanes
            cols = []
            for c in range(8):
                top = jnp.broadcast_to(tops[kd][:, off + c : off + c + 1], (8, lanes))
                tail = jnp.broadcast_to(tails[kd][:, off + c : off + c + 1], (rest, lanes)) if rest else None
                cols.append((top, tail))
            for c in range(8):
                top, tail = cols[c]
                inv = lax.rsqrt(top[c : c + 1, :])
                top = top * inv
                if rest:
                    tail = tail * inv
                for k in range(c + 1, 8):
                    scale = top[k : k + 1, :]
                    tk, lk = cols[k]
                    cols[k] = (tk - top * scale, lk - tail * scale if rest else None)
                for k in live:
                    row = tops[k][c : c + 1, :] * inv
                    tops[k] = jnp.where(sub == c, row, jnp.where(sub > c, tops[k] - top * row, tops[k]))
                    if rest:
                        tails[k] = tails[k] - tail * row
            for k in live:
                m_ref[j : j + 8, k * lanes : (k + 1) * lanes] = tops[k]
                if rest:
                    m_ref[j + 8 : end, k * lanes : (k + 1) * lanes] = tails[k]
        if end < n:
            first, last = live[0] * lanes, (live[-1] + 1) * lanes
            base = (end // lanes) * lanes
            update = lax.dot_general(
                m_ref[o:end, base:n], m_ref[o:end, first:last], TN,
                precision=lax.Precision.HIGHEST, preferred_element_type=F32,
            )
            m_ref[end:n, first:last] = m_ref[end:n, first:last] - update[end - base :, :]
    out_ref[...] = jnp.where(ri >= ci, m_ref[:, n:], 0.0)


def factor_inverse(gram, other):
    n = gram.shape[0]
    return pl.pallas_call(
        functools.partial(factor_kernel, n=n, outer=64),
        out_shape=jax.ShapeDtypeStruct((n, n), F32),
        scratch_shapes=[pltpu.VMEM((n, 2 * n), F32)],
        cost_estimate=cost(9),
        compiler_params=params(6),
        name="factor_inverse",
    )(gram, other)


def right_kernel(inv_ref, w_ref, other_ref, right_ref, pair_ref, inv_pair_ref, square_ref):
    inverse = inv_ref[...]
    rank = inverse.shape[0]
    right = dot3(split(inverse), split(w_ref[...] + other_ref[...]), MM)
    pair_ref[:rank, :], pair_ref[rank:, :] = split(right)
    inv_pair_ref[:rank, :], inv_pair_ref[rank:, :] = split(inverse.T)
    right = right.T
    right_ref[...] = right
    square_ref[...] = jnp.sum(right * right, axis=0, keepdims=True)


def right_part(inverse, weight, other):
    rank, cols = weight.shape
    return pl.pallas_call(
        right_kernel,
        out_shape=[
            jax.ShapeDtypeStruct((cols, rank), F32),
            jax.ShapeDtypeStruct((2 * rank, cols), BF16),
            jax.ShapeDtypeStruct((2 * rank, rank), BF16),
            jax.ShapeDtypeStruct((1, rank), F32),
        ],
        cost_estimate=cost(3),
        compiler_params=params(16),
        name="right_part",
    )(inverse, weight, other)


def momentum_kernel(m_ref, g_ref, left_ref, inv_ref, right_ref, *rest):
    out_ref, orth_ref = rest[-2:]
    rank = inv_ref.shape[1]
    orth = dot3(split(left_ref[...]), (inv_ref[:rank, :], inv_ref[rank:, :]), MM)
    orth_ref[...] = orth
    feedback = lax.dot_general(orth.astype(BF16), right_ref[...], MM, preferred_element_type=F32)
    out_ref[...] = m_ref[...] + g_ref[...].astype(F32) - FEEDBACK * feedback


def momentum_rows(momentum, gradient, left, inv_pair, pair, start, count, block, carry):
    rows, cols = momentum.shape
    rank = left.shape[1]
    row = lambda i: (start + i, 0)
    whole = lambda i: (0, 0)
    return pl.pallas_call(
        momentum_kernel,
        grid=(count,),
        in_specs=[
            pl.BlockSpec((block, cols), row),
            pl.BlockSpec((block, cols), row),
            pl.BlockSpec((block, rank), row),
            pl.BlockSpec((2 * rank, rank), whole),
            pl.BlockSpec((rank, cols), whole),
        ]
        + [pl.BlockSpec(memory_space=pl.ANY)] * len(carry),
        out_specs=[pl.BlockSpec((block, cols), row), pl.BlockSpec((block, rank), row)],
        out_shape=[jax.ShapeDtypeStruct((rows, cols), F32), jax.ShapeDtypeStruct((rows, rank), F32)],
        input_output_aliases={5 + k: k for k in range(len(carry))},
        cost_estimate=cost(4),
        compiler_params=params(20),
        name="momentum_rows",
    )(momentum, gradient, left, inv_pair, pair, *carry)


def update_kernel(core_ref, orth_ref, pair_ref, square_ref, share_ref, out_ref, next_ref, *, factor):
    norm = jnp.sqrt(square_ref[...] + EPS)
    rank = orth_ref.shape[1]

    @pl.when(pl.program_id(0) == 0)
    def _():
        next_ref[...] = share_ref[...] / norm

    orth = orth_ref[...] * (factor / norm)
    out_ref[...] = dot3(split(orth), (pair_ref[:rank, :], pair_ref[rank:, :]), MM).astype(BF16)


def update_rows(where, orth, pair, squares, right, share, factor, block):
    rows, rank = orth.shape
    cols = pair.shape[1]
    whole = lambda i, s: (0, 0)
    return pl.pallas_call(
        functools.partial(update_kernel, factor=factor),
        grid_spec=pltpu.PrefetchScalarGridSpec(
            num_scalar_prefetch=1,
            grid=(rows // block,),
            in_specs=[
                pl.BlockSpec((block, rank), lambda i, s: (i, 0)),
                pl.BlockSpec(pair.shape, whole),
                pl.BlockSpec(squares.shape, whole),
                pl.BlockSpec((share, rank), lambda i, s: (s[1], 0)),
            ],
            out_specs=[pl.BlockSpec((block, cols), lambda i, s: (i, 0)), pl.BlockSpec((share, rank), whole)],
        ),
        out_shape=[jax.ShapeDtypeStruct((rows, cols), BF16), jax.ShapeDtypeStruct((share, rank), F32)],
        cost_estimate=cost(5),
        compiler_params=params(20),
        name="update_rows",
    )(where, orth, pair, squares, right)


def swap(x, axis, size, step):
    return lax.ppermute(x, axis, [(i, i ^ step) for i in range(size)])


def row_rest(x, size):
    if size == 1:
        return jnp.zeros_like(x)
    total, step = swap(x, "row", size, 1), 2
    while step < size:
        whole = x + total
        total = total + swap(whole, "row", size, step)
        step *= 2
    return total


def groups_of(size):
    bits = size.bit_length() - 1
    groups, low = [], 2
    while low < bits:
        width = min(2, bits - low)
        groups.append((1 << low, 1 << width))
        low += width
    return groups


def scatter_sum(x, position, size):
    for step, members in groups_of(size):
        mine = (position // step) % members
        rows = x.shape[0] // members
        part = lambda k: lax.dynamic_slice_in_dim(x, k * rows, rows)
        got = [swap(part(mine ^ d), "col", size, d * step) for d in range(1, members)]
        x = part(mine)
        for piece in got:
            x = x + piece
    return x


def gather_rows(x, position, size):
    for step, members in reversed(groups_of(size)):
        mine = (position // step) % members
        pieces = [x] + [swap(x, "col", size, d * step) for d in range(1, members)]
        width = 1
        while width < members:
            odd = (mine // width) % 2 == 1
            pieces = [
                jnp.where(odd, jnp.concatenate([b, a]), jnp.concatenate([a, b]))
                for a, b in zip(pieces[0::2], pieces[1::2])
            ]
            width *= 2
        x = pieces[0]
    return x


def body(gradient, momentum, right_factor, *, cols_size, rows_size, factor):
    rows, cols = momentum.shape
    block = rows // 8
    half, quarter = rows // 2, rows // 4
    position = lax.axis_index("col")
    where = jnp.stack([position, lax.axis_index("row")]).astype(jnp.int32)
    if rows_size == 2:
        rest = swap(right_factor, "row", 2, 1)
    else:
        rest = lax.all_gather(right_factor, "row", axis=0, tiled=True)

    places = dict(
        near=lambda x, y: (x * quarter + y * block, half + y * quarter + x * block),
        side=lambda x, y: (x * quarter + (1 - y) * block, half + y * quarter + (1 - x) * block),
        cross=lambda x, y: ((1 - x) * quarter + y * block, half + (1 - y) * quarter + x * block),
        diagonal=lambda x, y: ((1 - x) * quarter + (1 - y) * block, half + (1 - y) * quarter + (1 - x) * block),
    )
    pieces = lambda name: left_rows(where, momentum, gradient, right_factor, rest, cols, block, places[name])
    along_x = lambda v: swap(v, "col", cols_size, 1)
    along_y = lambda v: swap(v, "col", cols_size, 2)
    send_a, send_b = pieces("diagonal")
    pass_a, pass_b = along_x(send_a), along_y(send_b)
    send_a, send_b = pieces("cross")
    got_a, got_b = along_x(send_a), along_y(send_b)
    keep_a, keep_b = pieces("side")
    pass_a, pass_b = along_y(pass_a + keep_a), along_x(pass_b + keep_b)
    keep_a, keep_b = pieces("near")
    own_a = keep_a + got_a + pass_a
    own_b = keep_b + got_b + pass_b
    own = jnp.concatenate([own_a.reshape(-1, block // (cols_size // 4), own_a.shape[1]),
                           own_b.reshape(-1, block // (cols_size // 4), own_b.shape[1])], axis=1)
    own = scatter_sum(own, position, cols_size)

    near = gather_rows(own, position, cols_size)
    cut = block // (cols_size // 4)
    near_a = near[:, :cut].reshape(block, -1)
    near_b = near[:, cut:].reshape(block, -1)
    side_a, side_b = along_y(near_a), along_x(near_b)
    cross_a, cross_b = along_x(near_a), along_y(near_b)
    diagonal_a, diagonal_b = along_x(side_a), along_y(side_b)
    weigh = functools.partial(weight_rows, where, momentum, gradient)
    carry = weigh(near_a, near_b, places["near"])
    carry = weigh(side_a, side_b, places["side"], carry)
    carry = weigh(cross_a, cross_b, places["cross"], carry)
    weight, gram, left = weigh(diagonal_a, diagonal_b, places["diagonal"], carry)

    gram_rest = row_rest(gram, rows_size)
    weight_rest = row_rest(weight, rows_size)
    inverse = factor_inverse(gram, gram_rest)
    right, pair, inv_pair, squares = right_part(inverse, weight, weight_rest)
    steps = cols_size.bit_length() - 1
    chunk = max(1, 8 // steps)
    carry, start = (), 0
    for k in range(steps):
        got = swap(squares, "col", cols_size, 1 << k)
        count = chunk if k + 1 < steps else 8 - start
        carry = momentum_rows(momentum, gradient, left, inv_pair, pair, start, count, block, carry)
        start += count
        got, *carry = lax.optimization_barrier((got, *carry))
        squares = squares + got
    momentum_next, orth = carry
    update, right_next = update_rows(where, orth, pair, squares, right, cols // rows_size, factor, 2 * block)
    return (momentum_next, right_next, update)


def solution(mesh):
    cols_size, rows_size = mesh.shape["col"], mesh.shape["row"]

    def step(gradient, momentum, right_factor):
        rows, cols = momentum.shape
        factor = math.sqrt(rows * cols / right_factor.shape[1])
        placed = (P("row", "col"), P("row", "col"), P(("col", "row"), None))
        return jax.shard_map(
            functools.partial(body, cols_size=cols_size, rows_size=rows_size, factor=factor),
            mesh=mesh,
            in_specs=placed,
            out_specs=(P("row", "col"), P(("col", "row"), None), P("row", "col")),
            check_vma=False,
        )(gradient, momentum, right_factor)

    return step
```

```python
import functools
import math

import jax
import jax.numpy as jnp
from jax import lax
from jax.experimental import pallas as pl
from jax.experimental.pallas import tpu as pltpu
from jax.sharding import PartitionSpec as P

EPS = 1e-06
FEEDBACK = 0.05
F32 = jnp.float32
BF16 = jnp.bfloat16


MM = (((1,), (0,)), ((), ()))
TN = (((0,), (0,)), ((), ()))
NT = (((1,), (1,)), ((), ()))


def split(x):
    high = x.astype(BF16)
    return high, (x - high.astype(F32)).astype(BF16)


def dot3(a, b, dims):
    (da,), (db,) = dims[0]
    left = jnp.concatenate([a[0], a[1], a[0]], axis=da)
    right = jnp.concatenate([b[0], b[0], b[1]], axis=db)
    return lax.dot_general(left, right, dims, preferred_element_type=F32)


def params(mib):
    return pltpu.CompilerParams(vmem_limit_bytes=mib << 20)


def cost(us):
    return pl.CostEstimate(flops=int(us * 1e9), bytes_accessed=1 << 20, transcendentals=0)


def left_kernel(
    where_ref, m_ref, g_ref, own_ref, rest_ref, a_ref, b_ref, m_buf, g_buf, own_buf, high_ref, low_ref, sems, *, starts, block
):
    position, own = where_ref[0], where_ref[1]
    copies = []
    for k, start in enumerate(starts(position % 2, (position // 2) % 2)):
        rows = pl.ds(pl.multiple_of(start, block), block)
        copies.append(
            (
                pltpu.make_async_copy(m_ref.at[rows], m_buf.at[k], sems.at[k, 0]),
                pltpu.make_async_copy(g_ref.at[rows], g_buf.at[k], sems.at[k, 1]),
            )
        )
    own_copy = pltpu.make_async_copy(own_ref, own_buf, sems.at[2, 0])
    own_copy.start()
    for pair in copies:
        for copy in pair:
            copy.start()
    own_copy.wait()

    share = own_ref.shape[0]
    for k in range(high_ref.shape[0] // share):
        rows = pl.ds(k * share, share)

        @pl.when(own == k)
        def _():
            high_ref[rows, :], low_ref[rows, :] = split(own_buf[...])

        @pl.when(own != k)
        def _():
            high_ref[rows, :], low_ref[rows, :] = split(rest_ref[rest_rows(rest_ref, share, k), :])

    for k, out_ref in enumerate((a_ref, b_ref)):
        for copy in copies[k]:
            copy.wait()
        blend = split(m_buf[k] + g_buf[k].astype(F32))
        out_ref[...] = dot3(blend, (high_ref[...], low_ref[...]), MM)


def rest_rows(rest_ref, share, k):
    return pl.ds(0 if rest_ref.shape[0] == share else k * share, share)


def block_map(starts, half, block):
    def at(i, s):
        a, b = starts(s[0] % 2, (s[0] // 2) % 2)
        return jnp.where(i < half, a // block + i, b // block + i - half), 0

    return at


def left_rows(where, momentum, gradient, own, rest, cols, block, starts):
    rank = own.shape[1]
    vmem, hbm = pl.BlockSpec(memory_space=pltpu.VMEM), pl.BlockSpec(memory_space=pltpu.HBM)
    return pl.pallas_call(
        functools.partial(left_kernel, starts=starts, block=block),
        in_specs=[pl.BlockSpec(memory_space=pltpu.SMEM), hbm, hbm, hbm, vmem],
        out_specs=[vmem, vmem],
        scratch_shapes=[
            pltpu.VMEM((2, block, cols), F32),
            pltpu.VMEM((2, block, cols), BF16),
            pltpu.VMEM(own.shape, F32),
            pltpu.VMEM((cols, rank), BF16),
            pltpu.VMEM((cols, rank), BF16),
            pltpu.SemaphoreType.DMA((3, 2)),
        ],
        out_shape=[jax.ShapeDtypeStruct((block, rank), F32), jax.ShapeDtypeStruct((block, rank), F32)],
        cost_estimate=cost(3),
        compiler_params=params(16),
        name="left_rows",
    )(where, *(pltpu.with_memory_space_constraint(v, pltpu.HBM) for v in (momentum, gradient, own)), rest)


def blend_kernel(m_ref, g_ref, out_ref):
    out_ref[...] = m_ref[...] + g_ref[...].astype(F32)


def blend_rows(momentum, gradient, block):
    rows, cols = momentum.shape
    spec = pl.BlockSpec((block, cols), lambda i: (i, 0))
    return pl.pallas_call(
        blend_kernel,
        grid=(rows // block,),
        in_specs=[spec, spec],
        out_specs=spec,
        out_shape=jax.ShapeDtypeStruct((rows, cols), F32),
        cost_estimate=cost(6),
        compiler_params=params(12),
        name="blend_rows",
    )(*(pltpu.with_memory_space_constraint(v, pltpu.HBM) for v in (momentum, gradient)))


def weight_kernel(at_ref, blend_ref, a_own, a_rest, b_own, b_rest, *rest, first):
    if first:
        w_ref, gram_ref, left_ref = rest
    else:
        w_in, gram_in, _, w_ref, gram_ref, left_ref = rest
    i = pl.program_id(0)

    @pl.when(i == 0)
    def _():
        if first:
            w_ref[...] = jnp.zeros_like(w_ref)
            gram_ref[...] = jnp.zeros_like(gram_ref)
        else:
            w_ref[...] = w_in[...]
            gram_ref[...] = gram_in[...]

    place, rows = (at_ref[0] // 4) % 4, a_own.shape[0]
    for k, (own, others) in enumerate(((a_own, a_rest), (b_own, b_rest))):

        @pl.when(i == k)
        def _():
            for d in range(4):
                to = pl.ds(pl.multiple_of((place ^ d) * rows, rows), rows)
                left_ref[to, :] = own[...] if d == 0 else others[(d - 1) * rows : d * rows, :]

    left = split(left_ref[...])
    w_ref[...] += dot3(left, split(blend_ref[...]), TN)
    gram_ref[...] += dot3(left, left, TN)


def weight_rows(where, blend, piece_a, piece_b, starts, carry=None):
    all_rows, cols = blend.shape
    rows, rank = piece_a[0].shape
    block = 4 * rows
    half, blocks = 1, 2
    at = block_map(starts, half, block)
    whole = lambda i, s: (0, 0)
    args = [blend, *piece_a, *piece_b]
    in_specs = [pl.BlockSpec((block, cols), at)] + [pl.BlockSpec(v.shape, whole) for v in args[1:]]
    aliases = {}
    if carry is not None:
        in_specs += [
            pl.BlockSpec((rank, cols), whole),
            pl.BlockSpec((rank, rank), whole),
            pl.BlockSpec(memory_space=pl.ANY),
        ]
        args += list(carry)
        aliases = {8: 2}
    return pl.pallas_call(
        functools.partial(weight_kernel, first=carry is None),
        grid_spec=pltpu.PrefetchScalarGridSpec(
            num_scalar_prefetch=1,
            grid=(blocks,),
            in_specs=in_specs,
            out_specs=[
                pl.BlockSpec((rank, cols), whole),
                pl.BlockSpec((rank, rank), whole),
                pl.BlockSpec((block, rank), at),
            ],
        ),
        out_shape=[
            jax.ShapeDtypeStruct((rank, cols), F32),
            jax.ShapeDtypeStruct((rank, rank), F32),
            jax.ShapeDtypeStruct((all_rows, rank), F32),
        ],
        input_output_aliases=aliases,
        cost_estimate=cost(2),
        compiler_params=params(30),
        name="weight_rows",
    )(where, *args)


def factor_kernel(gram_ref, other_ref, out_ref, m_ref, *, n, outer):
    lanes = 128
    chunks = n // lanes
    m_ref[:, :n] = gram_ref[...] + other_ref[...]
    ri = lax.broadcasted_iota(jnp.int32, (n, n), 0)
    ci = lax.broadcasted_iota(jnp.int32, (n, n), 1)
    m_ref[:, n:] = jnp.where(ri == ci, 1.0, 0.0).astype(F32)
    sub = lax.broadcasted_iota(jnp.int32, (8, lanes), 0)
    for o in range(0, n, outer):
        end = o + outer
        live = [k for k in range(chunks) if (k + 1) * lanes > o]
        live += [k + chunks for k in range(chunks) if k * lanes < end]
        for j in range(o, end, 8):
            rest = end - j - 8
            tops = {k: m_ref[j : j + 8, k * lanes : (k + 1) * lanes] for k in live}
            tails = {k: m_ref[j + 8 : end, k * lanes : (k + 1) * lanes] for k in live} if rest else {}
            kd, off = j // lanes, j % lanes
            cols = []
            for c in range(8):
                top = jnp.broadcast_to(tops[kd][:, off + c : off + c + 1], (8, lanes))
                tail = jnp.broadcast_to(tails[kd][:, off + c : off + c + 1], (rest, lanes)) if rest else None
                cols.append((top, tail))
            for c in range(8):
                top, tail = cols[c]
                inv = lax.rsqrt(top[c : c + 1, :])
                top = top * inv
                if rest:
                    tail = tail * inv
                for k in range(c + 1, 8):
                    scale = top[k : k + 1, :]
                    tk, lk = cols[k]
                    cols[k] = (tk - top * scale, lk - tail * scale if rest else None)
                for k in live:
                    row = tops[k][c : c + 1, :] * inv
                    tops[k] = jnp.where(sub == c, row, jnp.where(sub > c, tops[k] - top * row, tops[k]))
                    if rest:
                        tails[k] = tails[k] - tail * row
            for k in live:
                m_ref[j : j + 8, k * lanes : (k + 1) * lanes] = tops[k]
                if rest:
                    m_ref[j + 8 : end, k * lanes : (k + 1) * lanes] = tails[k]
        if end < n:
            first, last = live[0] * lanes, (live[-1] + 1) * lanes
            base = (end // lanes) * lanes
            update = lax.dot_general(
                m_ref[o:end, base:n], m_ref[o:end, first:last], TN,
                precision=lax.Precision.HIGHEST, preferred_element_type=F32,
            )
            m_ref[end:n, first:last] = m_ref[end:n, first:last] - update[end - base :, :]
    out_ref[...] = jnp.where(ri >= ci, m_ref[:, n:], 0.0)


def factor_inverse(gram, other):
    n = gram.shape[0]
    return pl.pallas_call(
        functools.partial(factor_kernel, n=n, outer=64),
        out_shape=jax.ShapeDtypeStruct((n, n), F32),
        scratch_shapes=[pltpu.VMEM((n, 2 * n), F32)],
        cost_estimate=cost(9),
        compiler_params=params(6),
        name="factor_inverse",
    )(gram, other)


def right_kernel(inv_ref, w_ref, other_ref, right_ref, pair_ref, inv_pair_ref, square_ref):
    inverse = inv_ref[...]
    rank = inverse.shape[0]
    right = dot3(split(inverse), split(w_ref[...] + other_ref[...]), MM)
    pair_ref[:rank, :], pair_ref[rank:, :] = split(right)
    inv_pair_ref[:rank, :], inv_pair_ref[rank:, :] = split(inverse.T)
    right = right.T
    right_ref[...] = right
    square_ref[...] = jnp.sum(right * right, axis=0, keepdims=True)


def right_part(inverse, weight, other):
    rank, cols = weight.shape
    return pl.pallas_call(
        right_kernel,
        out_shape=[
            jax.ShapeDtypeStruct((cols, rank), F32),
            jax.ShapeDtypeStruct((2 * rank, cols), BF16),
            jax.ShapeDtypeStruct((2 * rank, rank), BF16),
            jax.ShapeDtypeStruct((1, rank), F32),
        ],
        cost_estimate=cost(3),
        compiler_params=params(16),
        name="right_part",
    )(inverse, weight, other)


def momentum_kernel(blend_ref, left_ref, inv_ref, right_ref, *rest):
    out_ref, orth_ref = rest[-2:]
    rank = inv_ref.shape[1]
    orth = dot3(split(left_ref[...]), (inv_ref[:rank, :], inv_ref[rank:, :]), MM)
    orth_ref[...] = orth
    feedback = lax.dot_general(orth.astype(BF16), right_ref[...], MM, preferred_element_type=F32)
    out_ref[...] = blend_ref[...] - FEEDBACK * feedback


def momentum_rows(blend, left, inv_pair, pair, start, count, block, carry):
    rows, cols = blend.shape
    rank = left.shape[1]
    row = lambda i: (start + i, 0)
    whole = lambda i: (0, 0)
    return pl.pallas_call(
        momentum_kernel,
        grid=(count,),
        in_specs=[
            pl.BlockSpec((block, cols), row),
            pl.BlockSpec((block, rank), row),
            pl.BlockSpec((2 * rank, rank), whole),
            pl.BlockSpec((rank, cols), whole),
        ]
        + [pl.BlockSpec(memory_space=pl.ANY)] * len(carry),
        out_specs=[pl.BlockSpec((block, cols), row), pl.BlockSpec((block, rank), row)],
        out_shape=[jax.ShapeDtypeStruct((rows, cols), F32), jax.ShapeDtypeStruct((rows, rank), F32)],
        input_output_aliases={4 + k: k for k in range(len(carry))},
        cost_estimate=cost(4),
        compiler_params=params(20),
        name="momentum_rows",
    )(blend, left, inv_pair, pair, *carry)


def update_kernel(core_ref, orth_ref, pair_ref, square_ref, share_ref, out_ref, next_ref, *, factor):
    norm = jnp.sqrt(square_ref[...] + EPS)
    rank = orth_ref.shape[1]

    @pl.when(pl.program_id(0) == 0)
    def _():
        next_ref[...] = share_ref[...] / norm

    orth = orth_ref[...] * (factor / norm)
    out_ref[...] = dot3(split(orth), (pair_ref[:rank, :], pair_ref[rank:, :]), MM).astype(BF16)


def update_rows(where, orth, pair, squares, right, share, factor, block):
    rows, rank = orth.shape
    cols = pair.shape[1]
    whole = lambda i, s: (0, 0)
    return pl.pallas_call(
        functools.partial(update_kernel, factor=factor),
        grid_spec=pltpu.PrefetchScalarGridSpec(
            num_scalar_prefetch=1,
            grid=(rows // block,),
            in_specs=[
                pl.BlockSpec((block, rank), lambda i, s: (i, 0)),
                pl.BlockSpec(pair.shape, whole),
                pl.BlockSpec(squares.shape, whole),
                pl.BlockSpec((share, rank), lambda i, s: (s[1], 0)),
            ],
            out_specs=[pl.BlockSpec((block, cols), lambda i, s: (i, 0)), pl.BlockSpec((share, rank), whole)],
        ),
        out_shape=[jax.ShapeDtypeStruct((rows, cols), BF16), jax.ShapeDtypeStruct((share, rank), F32)],
        cost_estimate=cost(5),
        compiler_params=params(20),
        name="update_rows",
    )(where, orth, pair, squares, right)


def swap(x, axis, size, step):
    return lax.ppermute(x, axis, [(i, i ^ step) for i in range(size)])


def row_rest(x, size):
    if size == 1:
        return jnp.zeros_like(x)
    total, step = swap(x, "row", size, 1), 2
    while step < size:
        whole = x + total
        total = total + swap(whole, "row", size, step)
        step *= 2
    return total


def groups_of(size):
    bits = size.bit_length() - 1
    groups, low = [], 2
    while low < bits:
        width = min(2, bits - low)
        groups.append((1 << low, 1 << width))
        low += width
    return groups


def scatter_sum(x, position, size):
    for step, members in groups_of(size):
        mine = (position // step) % members
        rows = x.shape[0] // members
        part = lambda k: lax.dynamic_slice_in_dim(x, k * rows, rows)
        got = [swap(part(mine ^ d), "col", size, d * step) for d in range(1, members)]
        x = part(mine)
        for piece in got:
            x = x + piece
    return x


def gather_rows(x, position, size):
    for step, members in reversed(groups_of(size)[1:]):
        mine = (position // step) % members
        pieces = [x] + [swap(x, "col", size, d * step) for d in range(1, members)]
        width = 1
        while width < members:
            odd = (mine // width) % 2 == 1
            pieces = [
                jnp.where(odd, jnp.concatenate([b, a]), jnp.concatenate([a, b]))
                for a, b in zip(pieces[0::2], pieces[1::2])
            ]
            width *= 2
        x = pieces[0]
    return x


def body(gradient, momentum, right_factor, *, cols_size, rows_size, factor):
    rows, cols = momentum.shape
    block = rows // 8
    half, quarter = rows // 2, rows // 4
    position = lax.axis_index("col")
    where = jnp.stack([position, lax.axis_index("row")]).astype(jnp.int32)
    if rows_size == 2:
        rest = swap(right_factor, "row", 2, 1)
    else:
        rest = lax.all_gather(right_factor, "row", axis=0, tiled=True)

    places = dict(
        near=lambda x, y: (x * quarter + y * block, half + y * quarter + x * block),
        side=lambda x, y: (x * quarter + (1 - y) * block, half + y * quarter + (1 - x) * block),
        cross=lambda x, y: ((1 - x) * quarter + y * block, half + (1 - y) * quarter + x * block),
        diagonal=lambda x, y: ((1 - x) * quarter + (1 - y) * block, half + (1 - y) * quarter + (1 - x) * block),
    )
    pieces = lambda name: left_rows(where, momentum, gradient, right_factor, rest, cols, block, places[name])
    along_x = lambda v: swap(v, "col", cols_size, 1)
    along_y = lambda v: swap(v, "col", cols_size, 2)
    send_a, send_b = pieces("diagonal")
    pass_a, pass_b = along_x(send_a), along_y(send_b)
    send_a, send_b = pieces("cross")
    got_a, got_b = along_x(send_a), along_y(send_b)
    keep_a, keep_b = pieces("side")
    pass_a, pass_b = along_y(pass_a + keep_a), along_x(pass_b + keep_b)
    keep_a, keep_b = pieces("near")
    own_a = keep_a + got_a + pass_a
    own_b = keep_b + got_b + pass_b
    own = jnp.concatenate([own_a.reshape(-1, block // (cols_size // 4), own_a.shape[1]),
                           own_b.reshape(-1, block // (cols_size // 4), own_b.shape[1])], axis=1)
    momentum, gradient, own = lax.optimization_barrier((momentum, gradient, own))
    blend = blend_rows(momentum, gradient, block)
    own = scatter_sum(own, position, cols_size)
    own, blend = lax.optimization_barrier((own, blend))

    cut = block // (cols_size // 4)
    rows_a = lambda v: v[:, :cut].reshape(block // 4, -1)
    rows_b = lambda v: v[:, cut:].reshape(block // 4, -1)
    own = gather_rows(own, position, cols_size)
    others = [swap(own, "col", cols_size, 4 * d) for d in range(1, 4)]
    from_x, from_y = along_x(own), along_y(own)
    own_side = rows_a(from_y), rows_b(from_x)
    own_diagonal = along_x(own_side[0]), along_y(own_side[1])
    others, own_diagonal = lax.optimization_barrier((others, own_diagonal))
    near_a = jnp.concatenate([rows_a(v) for v in others])
    near_b = jnp.concatenate([rows_b(v) for v in others])
    side_a, side_b = along_y(near_a), along_x(near_b)
    cross_a, cross_b = along_x(near_a), along_y(near_b)
    diagonal_a, diagonal_b = along_x(side_a), along_y(side_b)
    weigh = functools.partial(weight_rows, where, blend)
    carry = weigh((rows_a(own), near_a), (rows_b(own), near_b), places["near"])
    carry = weigh((own_side[0], side_a), (own_side[1], side_b), places["side"], carry)
    carry = weigh((rows_a(from_x), cross_a), (rows_b(from_y), cross_b), places["cross"], carry)
    weight, gram, left = weigh(
        (own_diagonal[0], diagonal_a), (own_diagonal[1], diagonal_b), places["diagonal"], carry
    )

    gram_rest = row_rest(gram, rows_size)
    weight_rest = row_rest(weight, rows_size)
    inverse = factor_inverse(gram, gram_rest)
    right, pair, inv_pair, squares = right_part(inverse, weight, weight_rest)
    steps = cols_size.bit_length() - 1
    chunk = max(1, 8 // steps)
    carry, start = (), 0
    for k in range(steps):
        got = swap(squares, "col", cols_size, 1 << k)
        count = chunk if k + 1 < steps else 8 - start
        carry = momentum_rows(blend, left, inv_pair, pair, start, count, block, carry)
        start += count
        got, *carry = lax.optimization_barrier((got, *carry))
        squares = squares + got
    momentum_next, orth = carry
    update, right_next = update_rows(where, orth, pair, squares, right, cols // rows_size, factor, 2 * block)
    return (momentum_next, right_next, update)


def solution(mesh):
    cols_size, rows_size = mesh.shape["col"], mesh.shape["row"]

    def step(gradient, momentum, right_factor):
        rows, cols = momentum.shape
        factor = math.sqrt(rows * cols / right_factor.shape[1])
        placed = (P("row", "col"), P("row", "col"), P(("col", "row"), None))
        return jax.shard_map(
            functools.partial(body, cols_size=cols_size, rows_size=rows_size, factor=factor),
            mesh=mesh,
            in_specs=placed,
            out_specs=(P("row", "col"), P(("col", "row"), None), P("row", "col")),
            check_vma=False,
        )(gradient, momentum, right_factor)

    return step
```
